32 devices in a mesh: tile: 2 (over y), seq: 4 (over z), group: 4 (over x, core).
Axes of the slice: x: 2, y: 2, z: 4, core: 2. Of those that a mesh axis runs over, the one named last changes fastest.
Arguments:
- features: bfloat16 [4, 4, 2, 8, 64, 512], P('seq', 'group', None, 'tile'), may hold values from -6 to 6
- conv_weight: bfloat16 [3, 3, 3, 512, 16], replicated, may hold values from -0.0546875 to 0.0546875
- conv_bias: float32 [16], replicated, may hold values from -3 to 3
- embed_qkv: bfloat16 [64, 4608], replicated, may hold values from -0.75 to 0.75
- query_gain: float32 [128], replicated, may hold values from 0.5 to 2
- key_gain: float32 [128], replicated, may hold values from 0.5 to 2
- bucket: int32 [4, 4], replicated, may hold values from 0 to 3, as said below
- frames: int32 [4, 4], replicated, may hold values from 1 to 2
Outputs:
- attended: bfloat16 [4, 4, 2, 256, 1536], P('seq', 'group', None, 'tile')
The draws below stay inside these ranges and needn't reach their ends.
Inputs may be any that keep to these rules, and one draw needn't show every extreme that they name: In each row every bucket receives at most 2 clips; exactly 1 buckets receive 2, and as many receive none.
All inputs are finite; a program needn't handle non-finite values.
Results may differ from the reference program's by a relative error of at most 0.0046.
Values may be sent and summed in bfloat16 or wider, within the bound.
No kernel may reach another device: no remote copies, remote signals or barrier semaphores. Data moves between devices by JAX's collectives and lax.ppermute only.
A program may use at most 128 MiB of HBM per device.

```python
import math
import jax
import jax.numpy as jnp
from jax import lax

HEADS = 12
HEAD = 128
D = 1536
CH = 512
ZC = 16
TL = 2
HL = 4
WL = 64
CAP = 2
TOK = 128
TOKC = 256
N_TILE = 2
N_SEQ = 4
N_GROUP = 4


def draw_bucket(key, part):

    def one_row(row_key):
        first_key, second_key = jax.random.split(row_key)
        ranking = jax.random.permutation(first_key, N_GROUP)
        targets = jax.random.permutation(second_key, N_GROUP)
        paired = N_GROUP // 4
        position = jnp.where(ranking < 2 * paired, ranking // 2, ranking - paired)
        return targets[position]
    row_keys = jax.random.split(jax.random.fold_in(key, 7), N_SEQ)
    return jax.vmap(one_row)(row_keys).astype(jnp.int32)


def set_ends(array, rng, least, top_value):
    dims = array.shape
    index_at = [jax.random.randint(jax.random.fold_in(rng, axis), (), 0, dims[axis]) for axis in range(len(dims))]
    array = array.at[tuple(index_at)].set(least)
    longest = dims.index(max(dims))
    index_at[longest] = (index_at[longest] + 1) % dims[longest]
    return array.at[tuple(index_at)].set(top_value)


def steps_of(stream_key, dims, cuts, least, largest):
    gain = 1.0
    for axis_at, shards_of in cuts:
        steps = jax.random.uniform(jax.random.fold_in(jax.random.fold_in(stream_key, 6), axis_at), (shards_of,), jnp.float32, least / len(cuts), largest / len(cuts))
        gain = gain * jnp.repeat(jnp.exp(steps), dims[axis_at] // shards_of).reshape((-1,) + (1,) * (len(dims) - 1 - axis_at))
    return gain


def normal_values(stream_key, extent, width, bound, shards=(), kind=jnp.bfloat16):
    values = width * jax.random.normal(stream_key, extent, jnp.float32)
    if shards:
        values = values * steps_of(stream_key, extent, shards, -0.22, 0.18)
    return jnp.clip(values, -bound, bound).astype(kind)


def setup_inputs(seed: int = 0) -> dict:
    splits = jax.random.split(jax.random.key(seed), 9)
    return {
        "features": normal_values(splits[0], (N_SEQ, N_GROUP, TL, N_TILE * HL, WL, CH), 1.0, 6.0, ((0, 4), (1, 4), (3, 2))),
        "conv_weight": normal_values(splits[1], (3, 3, 3, CH, ZC), (27 * CH) ** -0.5, 0.0546875),
        "conv_bias": normal_values(splits[2], (ZC,), 0.5, 3.0, (), jnp.float32),
        "embed_qkv": normal_values(splits[3], (4 * ZC, 3 * D), (4 * ZC) ** -0.5, 0.75),
        "query_gain": jnp.clip(jnp.exp(jax.random.uniform(splits[4], (HEAD,), jnp.float32, math.log(0.5), math.log(2.0))), 0.5, 2.0),
        "key_gain": jnp.clip(jnp.exp(jax.random.uniform(splits[5], (HEAD,), jnp.float32, math.log(0.5), math.log(2.0))), 0.5, 2.0),
        "bucket": draw_bucket(jax.random.fold_in(splits[8], 71), 0),
        "frames": set_ends(jax.random.randint(splits[7], (N_SEQ, N_GROUP), 1, TL + 1), jax.random.fold_in(splits[7], 1), 1, TL).astype(jnp.int32),
    }


def tap_products(padded, conv_weight):
    channels = padded.shape[-1]
    flat_weight = jnp.transpose(conv_weight, (3, 0, 1, 2, 4)).reshape(channels, -1)
    products = jnp.dot(padded.reshape(-1, channels), flat_weight, preferred_element_type=jnp.float32)
    return products.reshape(padded.shape[:-1] + (27, conv_weight.shape[-1]))

def tap_sum(products, frame_count, row_count, col_count):
    running = jnp.zeros((frame_count, row_count, col_count, products.shape[-1]), jnp.float32)
    for depth_tap in range(3):
        for row_tap in range(3):
            for col_tap in range(3):
                tap_index = depth_tap * 9 + row_tap * 3 + col_tap
                running = running + products[depth_tap:depth_tap + frame_count, row_tap:row_tap + row_count, col_tap:col_tap + col_count, tap_index]
    return running

def head_norm(values, gain_vec, head_size):
    shaped = values.reshape(values.shape[:-1] + (-1, head_size))
    scaled = shaped * lax.rsqrt(lax.optimization_barrier(jnp.mean(shaped * shaped, axis=-1, keepdims=True)) + 1e-06)
    return scaled * gain_vec

def attend(queries, key_rows, value_rows, key_valid):
    query_wide = lax.optimization_barrier(queries).astype(jnp.float32)
    key_wide = lax.optimization_barrier(key_rows).astype(jnp.float32)
    value_wide = lax.optimization_barrier(value_rows).astype(jnp.float32)
    scores = jnp.einsum('qhe,khe->hqk', query_wide, key_wide)
    scores = jnp.where(key_valid[None, None, :], scores, -1e+30)
    row_max = lax.optimization_barrier(jnp.max(scores, axis=-1, keepdims=True))
    weights = jnp.exp(scores - row_max)
    totals = lax.optimization_barrier(jnp.sum(weights, axis=-1))
    weight_low = lax.optimization_barrier(weights.astype(jnp.bfloat16)).astype(jnp.float32)
    mixed_out = jnp.einsum('hqk,khe->qhe', weight_low, value_wide)
    return mixed_out / jnp.transpose(totals)[:, :, None]

def reference(features, conv_weight, conv_bias, embed_qkv, query_gain, key_gain, bucket, frames):
    clips = features.reshape((N_SEQ * N_GROUP,) + features.shape[2:])

    def encode_attend(pair):
        clip_block, frame_total = pair
        padded = jnp.pad(clip_block, ((2, 0), (1, 1), (1, 1), (0, 0)), mode='edge')
        summed = tap_sum(tap_products(padded, conv_weight), TL, N_TILE * HL, WL)
        latent = (summed + conv_bias).astype(jnp.bfloat16)
        tokens = latent.reshape(TL, N_TILE, HL // 2, 2, WL // 2, 2, ZC)
        tokens = jnp.transpose(tokens, (1, 0, 2, 4, 3, 5, 6)).reshape(-1, 4 * ZC)
        projected = jnp.dot(tokens, embed_qkv, preferred_element_type=jnp.float32)
        queries = (head_norm(projected[:, :D], query_gain, HEAD) / math.sqrt(HEAD)).astype(jnp.bfloat16)
        key_rows = head_norm(projected[:, D:2 * D], key_gain, HEAD).astype(jnp.bfloat16)
        value_rows = projected[:, 2 * D:].reshape(-1, HEADS, HEAD).astype(jnp.bfloat16)
        frame_of = jnp.arange(TOKC, dtype=jnp.int32) % TOK // (HL // 2 * (WL // 2))
        valid = frame_of < frame_total
        mixed_out = attend(queries, key_rows, value_rows, valid)
        return jnp.where(valid[:, None], mixed_out.reshape(-1, D), 0.0).astype(jnp.bfloat16)
    results = lax.map(encode_attend, (clips, frames.reshape(-1)))
    order_ids = jnp.arange(N_GROUP, dtype=jnp.int32)
    same_bucket = bucket[:, :, None] == bucket[:, None, :]
    earlier = order_ids[None, None, :] < order_ids[None, :, None]
    slot_of = lax.optimization_barrier(jnp.sum(jnp.where(same_bucket & earlier, 1, 0), axis=2)).astype(jnp.int32)
    slot_ids = jnp.arange(CAP, dtype=jnp.int32)
    matches = (bucket[:, None, None, :] == order_ids[None, :, None, None]) & (slot_of[:, None, None, :] == slot_ids[None, None, :, None])
    source = lax.optimization_barrier(jnp.sum(jnp.where(matches, order_ids[None, None, None, :], 0), axis=3)).astype(jnp.int32)
    present = jnp.any(matches, axis=3)
    flat_index = (jnp.arange(N_SEQ, dtype=jnp.int32)[:, None, None] * N_GROUP + source).astype(jnp.int32)
    placed = results[flat_index]
    return jnp.where(present[:, :, :, None, None], placed, jnp.zeros((), jnp.bfloat16))
```

```python
import functools
import math

import jax
import jax.numpy as jnp
from jax import lax
from jax.experimental import pallas as pl
from jax.experimental.pallas import tpu as pltpu
from jax.sharding import PartitionSpec as P

HEADS = 12
HEAD = 128
D = 1536
CAP = 2
EPS = 1e-06
BF16 = jnp.bfloat16
F32 = jnp.float32

VMEM = pl.BlockSpec(memory_space=pltpu.VMEM)
SMEM = pl.BlockSpec(memory_space=pltpu.SMEM)
HBM = pl.BlockSpec(memory_space=pltpu.HBM)


def in_vmem(*arrays):
    return [pltpu.with_memory_space_constraint(array, pltpu.VMEM) for array in arrays]


def column(row):
    size = row.shape[1]
    wide = jnp.broadcast_to(row, (size, size))
    down = lax.broadcasted_iota(jnp.int32, (size, size), 0)
    across = lax.broadcasted_iota(jnp.int32, (size, size), 1)
    return jnp.sum(jnp.where(down == across, wide, 0.0), axis=1, keepdims=True)


def conv_rows(features_ref, weight_ref, bias_ref, x_scr, w_scr, x_sem, w_sem, tiles):
    _, _, frames, rows, cols, _ = features_ref.shape
    lanes = frames * cols
    w_copy = pltpu.make_async_copy(weight_ref, w_scr, w_sem)
    w_copy.start()
    copies = []
    for row in range(rows):
        copy = pltpu.make_async_copy(features_ref.at[0, 0, :, row], x_scr.at[row], x_sem.at[row])
        copy.start()
        copies.append(copy)
    tile = lax.axis_index("tile")
    is_first = tile == 0
    is_last = tile == tiles - 1
    lane = lax.broadcasted_iota(jnp.int32, (16, lanes), 1)
    col = lane % cols
    in_first = lane < cols
    w_copy.wait()
    taps = []
    for pair in range(rows // 2):
        copies[2 * pair].wait()
        copies[2 * pair + 1].wait()
        block = x_scr[2 * pair : 2 * pair + 2].reshape(2 * lanes, -1)
        products = lax.dot_general(
            w_scr[...], block, (((1,), (1,)), ((), ())), preferred_element_type=F32
        )
        for half in range(2):
            part = products[:, half * lanes : (half + 1) * lanes]
            row_taps = []
            for b in range(3):
                row_taps.append([])
                for c in range(3):
                    tap = [part[(a * 9 + b * 3 + c) * 16 : (a * 9 + b * 3 + c + 1) * 16] for a in range(3)]
                    row_taps[b].append((tap[0] + tap[1], tap[2]))
            taps.append(row_taps)

    def finish(sums):
        def shifted(value, c):
            if c == 0:
                return jnp.where(col == 0, value, pltpu.roll(value, 1, 1))
            if c == 2:
                return jnp.where(col == cols - 1, value, pltpu.roll(value, lanes - 1, 1))
            return value

        early = sum(shifted(sums[c][0], c) for c in range(3))
        late = sum(shifted(sums[c][1], c) for c in range(3))
        return late + jnp.where(in_first, early, pltpu.roll(early, cols, 1))

    def add(*parts):
        return [tuple(sum(p[c][k] for p in parts) for k in range(2)) for c in range(3)]

    bias = column(bias_ref[...])
    out = []
    for row in range(rows):
        parts = [taps[row + b - 1][b] for b in range(3) if 0 <= row + b - 1 < rows]
        value = finish(add(*parts)) + bias
        if row == 0:
            value = value + jnp.where(is_first, finish(taps[0][0]), 0.0)
        if row == rows - 1:
            value = value + jnp.where(is_last, finish(taps[rows - 1][2]), 0.0)
        out.append(value)
    return out, finish(taps[rows - 1][0]), finish(taps[0][2]), is_first


def conv_pair_kernel(features_ref, weight_ref, bias_ref, send_ref, keep_ref, x_scr, w_scr, x_sem, w_sem):
    out, below, above, is_first = conv_rows(
        features_ref, weight_ref, bias_ref, x_scr, w_scr, x_sem, w_sem, 2
    )
    rows = len(out)
    for row in range(rows):
        send_ref[row] = out[row].astype(BF16)
    edge = jnp.where(is_first, out[rows - 1], out[0])
    owed = jnp.where(is_first, below, above)
    keep_ref[0] = edge
    keep_ref[1] = owed
    send_ref[rows] = (edge - edge.astype(BF16).astype(F32)).astype(BF16)
    high = owed.astype(BF16)
    send_ref[rows + 1] = high
    send_ref[rows + 2] = (owed - high.astype(F32)).astype(BF16)


def selection(lanes, cols):
    shape = (2 * lanes, 2 * lanes)
    src = lax.broadcasted_iota(jnp.int32, shape, 0)
    dst = lax.broadcasted_iota(jnp.int32, shape, 1)
    half = cols // 2
    x = dst // lanes
    f = dst % lanes // cols
    i = dst % cols // half
    j = dst % half
    want = i * lanes + f * cols + 2 * j + x
    return jnp.where(src == want, 1.0, 0.0).astype(BF16)


def to_tokens(latent_rows, cols):
    blocks = [
        jnp.concatenate([latent_rows[y], latent_rows[2 + y]], axis=1) for y in range(2)
    ]
    return jnp.concatenate(blocks, axis=0)


def finish_pair_kernel(send_ref, recv_ref, keep_ref, tokens_ref, *, cols):
    is_first = lax.axis_index("tile") == 0
    slots, zc, lanes = send_ref.shape
    rows = slots - 3
    mine = [send_ref[row].astype(F32) for row in range(rows)]
    theirs = [recv_ref[row].astype(F32) for row in range(rows)]
    my_edge = keep_ref[0] + (recv_ref[rows + 1].astype(F32) + recv_ref[rows + 2].astype(F32))
    their_edge = jnp.where(is_first, theirs[0], theirs[rows - 1]) + recv_ref[rows].astype(F32) + keep_ref[1]
    mine[0] = jnp.where(is_first, mine[0], my_edge)
    mine[rows - 1] = jnp.where(is_first, my_edge, mine[rows - 1])
    theirs[0] = jnp.where(is_first, their_edge, theirs[0])
    theirs[rows - 1] = jnp.where(is_first, theirs[rows - 1], their_edge)
    low = [jnp.where(is_first, a, b) for a, b in zip(mine, theirs)]
    high = [jnp.where(is_first, b, a) for a, b in zip(mine, theirs)]
    stacked = jnp.concatenate([to_tokens(low, cols), to_tokens(high, cols)], axis=0).astype(BF16)
    picked = jnp.dot(stacked, selection(lanes, cols), preferred_element_type=F32).astype(BF16)
    for t in range(2):
        for y in range(2):
            for x in range(2):
                tokens_ref[t, (2 * y + x) * zc : (2 * y + x + 1) * zc] = picked[
                    (2 * t + y) * zc : (2 * t + y + 1) * zc, x * lanes : (x + 1) * lanes
                ]


def conv_any_kernel(features_ref, weight_ref, bias_ref, part_ref, owed_ref, x_scr, w_scr, x_sem, w_sem, *, tiles):
    out, below, above, _ = conv_rows(
        features_ref, weight_ref, bias_ref, x_scr, w_scr, x_sem, w_sem, tiles
    )
    for row, value in enumerate(out):
        part_ref[row] = value
    owed_ref[0] = below
    owed_ref[1] = above


def finish_any_kernel(part_ref, from_low_ref, from_high_ref, tokens_ref, *, cols):
    rows, zc, lanes = part_ref.shape
    latent = [part_ref[row] for row in range(rows)]
    latent[0] = latent[0] + from_low_ref[...]
    latent[rows - 1] = latent[rows - 1] + from_high_ref[...]
    stacked = to_tokens(latent, cols).astype(BF16)
    picked = jnp.dot(stacked, selection(lanes, cols), preferred_element_type=F32).astype(BF16)
    for y in range(2):
        for x in range(2):
            tokens_ref[(2 * y + x) * zc : (2 * y + x + 1) * zc] = picked[
                y * zc : (y + 1) * zc, x * lanes : (x + 1) * lanes
            ]


def prepare_kernel(embed_ref, qgain_ref, kgain_ref, key_t_ref, qscale_ref, kscale_ref):
    key_t_ref[...] = jnp.transpose(embed_ref[:, D : 2 * D].astype(F32)).astype(BF16)
    qscale_ref[...] = qgain_ref[...] * (math.log2(math.e) / math.sqrt(HEAD))
    kscale_ref[...] = jnp.broadcast_to(column(kgain_ref[...]), kscale_ref.shape)


def attend_kernel(*refs, groups, sources, cols):
    bucket_ref, frames_ref = refs[:2]
    token_refs = refs[2 : 2 + sources]
    embed_ref, key_t_ref, qscale_ref, kscale_ref, out_ref = refs[2 + sources : 7 + sources]
    nat_scr, out_scr, sem = refs[7 + sources :]
    seq = lax.axis_index("seq")
    me = lax.axis_index("group")
    tile = lax.axis_index("tile")
    tiles, feat, lanes = token_refs[0].shape[-3:]
    clip = tiles * lanes
    src = [jnp.int32(0)] * CAP
    count = jnp.int32(0)
    for g in range(groups):
        hit = bucket_ref[seq, g] == me
        for slot in range(CAP):
            src[slot] = jnp.where(hit & (count == slot), g, src[slot])
        count = count + jnp.where(hit, 1, 0)

    query_gain = qscale_ref[...]
    key_gain = kscale_ref[...]
    frame_lane = lax.broadcasted_iota(jnp.int32, (1, lanes), 1) // cols
    frame_row = lax.broadcasted_iota(jnp.int32, (lanes, 1), 0) // cols
    copies = []
    for slot in range(CAP):
        filled = count > slot
        total = jnp.where(filled, frames_ref[seq, src[slot]], 0)
        if sources == 1:
            raw = token_refs[0][src[slot]].astype(F32)
        else:
            at = src[slot] ^ me
            raw = token_refs[0][...].astype(F32)
            for k in range(1, sources):
                raw = jnp.where(at == k, token_refs[k][...].astype(F32), raw)
        valid = jnp.where(frame_lane < total, 1.0, 0.0)
        counted = jnp.where(frame_lane < jnp.maximum(total, 1), 1.0, 0.0)
        row_keep = jnp.where(frame_row < total, 1.0, 0.0)
        tokens_t = jnp.concatenate([raw[t] * valid for t in range(tiles)], axis=1)
        nat_scr[slot] = jnp.transpose(tokens_t).astype(BF16)
        tokens_t = tokens_t.astype(BF16)
        natural = nat_scr[slot]
        mine = nat_scr[slot, pl.ds(pl.multiple_of(tile * lanes, lanes), lanes), :]
        for pair in range(HEADS // 2):
            span = slice(pair * 2 * HEAD, (pair + 1) * 2 * HEAD)
            keys = jnp.dot(key_t_ref[span, :], tokens_t, preferred_element_type=F32)
            queries = jnp.dot(mine, embed_ref[:, span], preferred_element_type=F32)
            values = jnp.dot(
                natural, embed_ref[:, 2 * D + span.start : 2 * D + span.stop], preferred_element_type=F32
            ).astype(BF16)
            for half in range(2):
                one = slice(half * HEAD, (half + 1) * HEAD)
                k = keys[one]
                k = k * lax.rsqrt(jnp.mean(k * k, axis=0, keepdims=True) + EPS) * key_gain
                q = queries[:, one]
                q = q * lax.rsqrt(jnp.mean(q * q, axis=1, keepdims=True) + EPS) * query_gain
                scores = jnp.dot(q.astype(BF16), k.astype(BF16), preferred_element_type=F32)
                weights = jnp.exp2(scores)
                folded = weights[:, :lanes]
                for t in range(1, tiles):
                    folded = folded + weights[:, t * lanes : (t + 1) * lanes]
                totals = jnp.sum(folded * counted, axis=1, keepdims=True)
                mixed = jnp.dot(weights.astype(BF16), values[:, one], preferred_element_type=F32)
                head = 2 * pair + half
                out_scr[slot, :, head * HEAD : (head + 1) * HEAD] = (
                    mixed * (row_keep / totals)
                ).astype(BF16)
        copy = pltpu.make_async_copy(out_scr.at[slot], out_ref.at[slot], sem.at[slot])
        copy.start()
        copies.append(copy)
    for copy in copies:
        copy.wait()


def clip_tokens(features, weight_t, bias_row):
    _, _, frames, rows, cols, channels = features.shape
    zc = bias_row.shape[1]
    lanes = frames * cols
    tiles = lax.axis_size("tile")
    scratch = [
        pltpu.VMEM((rows, frames, cols, channels), BF16),
        pltpu.VMEM(weight_t.shape, BF16),
        pltpu.SemaphoreType.DMA((rows,)),
        pltpu.SemaphoreType.DMA,
    ]
    if tiles == 2:
        send, keep = pl.pallas_call(
            conv_pair_kernel,
            out_shape=(pltpu.VMEM((rows + 3, zc, lanes), BF16), pltpu.VMEM((2, zc, lanes), F32)),
            in_specs=[HBM, HBM, VMEM],
            out_specs=(VMEM, VMEM),
            scratch_shapes=scratch,
            name="conv",
        )(features, weight_t, bias_row)
        recv = lax.ppermute(send, "tile", [(0, 1), (1, 0)])
        return pl.pallas_call(
            functools.partial(finish_pair_kernel, cols=cols),
            out_shape=pltpu.VMEM((2, 4 * zc, lanes), BF16),
            in_specs=[VMEM, VMEM, VMEM],
            out_specs=VMEM,
            name="finish",
        )(*in_vmem(send, recv, keep))
    part, owed = pl.pallas_call(
        functools.partial(conv_any_kernel, tiles=tiles),
        out_shape=(pltpu.VMEM((rows, zc, lanes), F32), pltpu.VMEM((2, zc, lanes), F32)),
        in_specs=[HBM, HBM, VMEM],
        out_specs=(VMEM, VMEM),
        scratch_shapes=scratch,
        name="conv",
    )(features, weight_t, bias_row)
    up = [(i, i + 1) for i in range(tiles - 1)]
    from_low = lax.ppermute(owed[0], "tile", up)
    from_high = lax.ppermute(owed[1], "tile", [(b, a) for a, b in up])
    tokens = pl.pallas_call(
        functools.partial(finish_any_kernel, cols=cols),
        out_shape=pltpu.VMEM((4 * zc, lanes), BF16),
        in_specs=[VMEM, VMEM, VMEM],
        out_specs=VMEM,
        name="finish",
    )(*in_vmem(part, from_low, from_high))
    return lax.all_gather(tokens, "tile", axis=0)


def shards(features, conv_weight, conv_bias, embed_qkv, query_gain, key_gain, bucket, frames):
    _, _, frame_count, rows, cols, channels = features.shape
    zc = conv_weight.shape[-1]
    lanes = frame_count * cols
    tiles = lax.axis_size("tile")
    groups = lax.axis_size("group")
    weight_t = jnp.transpose(conv_weight, (0, 1, 2, 4, 3)).reshape(-1, channels)
    tokens = clip_tokens(features, weight_t, conv_bias.reshape(1, -1))
    (embed,) = in_vmem(embed_qkv)
    key_t, query_scale, key_scale = pl.pallas_call(
        prepare_kernel,
        out_shape=(
            pltpu.VMEM((D, 4 * zc), BF16),
            pltpu.VMEM((1, HEAD), F32),
            pltpu.VMEM((HEAD, tiles * lanes), F32),
        ),
        in_specs=[VMEM, VMEM, VMEM],
        out_specs=(VMEM, VMEM, VMEM),
        name="prepare",
    )(embed, query_gain.reshape(1, -1), key_gain.reshape(1, -1))
    if groups in (2, 4):
        sources = [tokens] + [
            lax.ppermute(tokens, "group", [(i, i ^ k) for i in range(groups)]) for k in range(1, groups)
        ]
    else:
        sources = [lax.all_gather(tokens, "group", axis=0)]
    out = pl.pallas_call(
        functools.partial(attend_kernel, groups=groups, sources=len(sources), cols=cols),
        out_shape=jax.ShapeDtypeStruct((CAP, lanes, D), BF16),
        in_specs=[SMEM, SMEM] + [VMEM] * (len(sources) + 4),
        out_specs=HBM,
        scratch_shapes=[
            pltpu.VMEM((CAP, tiles * lanes, 4 * zc), BF16),
            pltpu.VMEM((CAP, lanes, D), BF16),
            pltpu.SemaphoreType.DMA((CAP,)),
        ],
        name="attend",
    )(bucket, frames, *in_vmem(*sources, embed, key_t, query_scale, key_scale))
    return out[None, None]


def solution(mesh):
    in_specs = (P("seq", "group", None, "tile", None, None), P(), P(), P(), P(), P(), P(), P())
    out_specs = P("seq", "group", None, "tile", None)
    return jax.shard_map(shards, mesh=mesh, in_specs=in_specs, out_specs=out_specs, check_vma=False)
```

```python
import functools
import math

import jax
import jax.numpy as jnp
from jax import lax
from jax.experimental import pallas as pl
from jax.experimental.pallas import tpu as pltpu
from jax.sharding import PartitionSpec as P

HEADS = 12
HEAD = 128
D = 1536
CAP = 2
EPS = 1e-06
BF16 = jnp.bfloat16
F32 = jnp.float32

VMEM = pl.BlockSpec(memory_space=pltpu.VMEM)
SMEM = pl.BlockSpec(memory_space=pltpu.SMEM)
HBM = pl.BlockSpec(memory_space=pltpu.HBM)


def in_vmem(*arrays):
    return [pltpu.with_memory_space_constraint(array, pltpu.VMEM) for array in arrays]


def column(row):
    size = row.shape[1]
    wide = jnp.broadcast_to(row, (size, size))
    down = lax.broadcasted_iota(jnp.int32, (size, size), 0)
    across = lax.broadcasted_iota(jnp.int32, (size, size), 1)
    return jnp.sum(jnp.where(down == across, wide, 0.0), axis=1, keepdims=True)


def conv_rows(features_ref, weight_ref, bias_ref, x_scr, w_scr, b_scr, x_sem, w_sem, b_sem, tiles):
    _, _, frames, rows, cols, _ = features_ref.shape
    lanes = frames * cols
    w_copy = pltpu.make_async_copy(weight_ref, w_scr, w_sem)
    w_copy.start()
    copies = []
    for row in range(rows):
        copy = pltpu.make_async_copy(features_ref.at[0, 0, :, row], x_scr.at[row], x_sem.at[row])
        copy.start()
        copies.append(copy)
    b_copy = pltpu.make_async_copy(bias_ref, b_scr, b_sem)
    b_copy.start()
    tile = lax.axis_index("tile")
    is_first = tile == 0
    is_last = tile == tiles - 1
    lane = lax.broadcasted_iota(jnp.int32, (16, lanes), 1)
    col = lane % cols
    in_first = lane < cols
    b_copy.wait()
    bias = column(b_scr[...])
    w_copy.wait()
    taps = []
    for pair in range(rows // 2):
        copies[2 * pair].wait()
        copies[2 * pair + 1].wait()
        block = x_scr[2 * pair : 2 * pair + 2].reshape(2 * lanes, -1)
        products = lax.dot_general(
            w_scr[...], block, (((1,), (1,)), ((), ())), preferred_element_type=F32
        )
        for half in range(2):
            part = products[:, half * lanes : (half + 1) * lanes]
            row_taps = []
            for b in range(3):
                row_taps.append([])
                for c in range(3):
                    tap = [part[(a * 9 + b * 3 + c) * 16 : (a * 9 + b * 3 + c + 1) * 16] for a in range(3)]
                    row_taps[b].append((tap[0] + tap[1], tap[2]))
            taps.append(row_taps)

    def finish(sums):
        def shifted(value, c):
            if c == 0:
                return jnp.where(col == 0, value, pltpu.roll(value, 1, 1))
            if c == 2:
                return jnp.where(col == cols - 1, value, pltpu.roll(value, lanes - 1, 1))
            return value

        early = sum(shifted(sums[c][0], c) for c in range(3))
        late = sum(shifted(sums[c][1], c) for c in range(3))
        return late + jnp.where(in_first, early, pltpu.roll(early, cols, 1))

    def add(*parts):
        return [tuple(sum(p[c][k] for p in parts) for k in range(2)) for c in range(3)]

    out = []
    for row in range(rows):
        parts = [taps[row + b - 1][b] for b in range(3) if 0 <= row + b - 1 < rows]
        value = finish(add(*parts)) + bias
        if row == 0:
            value = value + jnp.where(is_first, finish(taps[0][0]), 0.0)
        if row == rows - 1:
            value = value + jnp.where(is_last, finish(taps[rows - 1][2]), 0.0)
        out.append(value)
    return out, finish(taps[rows - 1][0]), finish(taps[0][2]), is_first


def conv_pair_kernel(features_ref, weight_ref, bias_ref, send_ref, keep_ref, *scratch):
    out, below, above, is_first = conv_rows(features_ref, weight_ref, bias_ref, *scratch, 2)
    rows = len(out)
    for row in range(rows):
        send_ref[row] = out[row].astype(BF16)
    edge = jnp.where(is_first, out[rows - 1], out[0])
    owed = jnp.where(is_first, below, above)
    keep_ref[0] = edge
    keep_ref[1] = owed
    send_ref[rows] = (edge - edge.astype(BF16).astype(F32)).astype(BF16)
    high = owed.astype(BF16)
    send_ref[rows + 1] = high
    send_ref[rows + 2] = (owed - high.astype(F32)).astype(BF16)


def selection(lanes, cols):
    shape = (2 * lanes, 2 * lanes)
    src = lax.broadcasted_iota(jnp.int32, shape, 0)
    dst = lax.broadcasted_iota(jnp.int32, shape, 1)
    half = cols // 2
    x = dst // lanes
    f = dst % lanes // cols
    i = dst % cols // half
    j = dst % half
    want = i * lanes + f * cols + 2 * j + x
    return jnp.where(src == want, 1.0, 0.0).astype(BF16)


def to_tokens(latent_rows, cols):
    blocks = [
        jnp.concatenate([latent_rows[y], latent_rows[2 + y]], axis=1) for y in range(2)
    ]
    return jnp.concatenate(blocks, axis=0)


def finish_pair_kernel(send_ref, recv_ref, keep_ref, tokens_ref, *, cols):
    is_first = lax.axis_index("tile") == 0
    slots, zc, lanes = send_ref.shape
    rows = slots - 3
    mine = [send_ref[row].astype(F32) for row in range(rows)]
    theirs = [recv_ref[row].astype(F32) for row in range(rows)]
    my_edge = keep_ref[0] + (recv_ref[rows + 1].astype(F32) + recv_ref[rows + 2].astype(F32))
    their_edge = jnp.where(is_first, theirs[0], theirs[rows - 1]) + recv_ref[rows].astype(F32) + keep_ref[1]
    mine[0] = jnp.where(is_first, mine[0], my_edge)
    mine[rows - 1] = jnp.where(is_first, my_edge, mine[rows - 1])
    theirs[0] = jnp.where(is_first, their_edge, theirs[0])
    theirs[rows - 1] = jnp.where(is_first, theirs[rows - 1], their_edge)
    low = [jnp.where(is_first, a, b) for a, b in zip(mine, theirs)]
    high = [jnp.where(is_first, b, a) for a, b in zip(mine, theirs)]
    stacked = jnp.concatenate([to_tokens(low, cols), to_tokens(high, cols)], axis=0).astype(BF16)
    picked = jnp.dot(stacked, selection(lanes, cols), preferred_element_type=F32).astype(BF16)
    for t in range(2):
        for y in range(2):
            for x in range(2):
                tokens_ref[t, (2 * y + x) * zc : (2 * y + x + 1) * zc] = picked[
                    (2 * t + y) * zc : (2 * t + y + 1) * zc, x * lanes : (x + 1) * lanes
                ]


def conv_any_kernel(features_ref, weight_ref, bias_ref, part_ref, owed_ref, *scratch, tiles):
    out, below, above, _ = conv_rows(features_ref, weight_ref, bias_ref, *scratch, tiles)
    for row, value in enumerate(out):
        part_ref[row] = value
    owed_ref[0] = below
    owed_ref[1] = above


def finish_any_kernel(part_ref, from_low_ref, from_high_ref, tokens_ref, *, cols):
    rows, zc, lanes = part_ref.shape
    latent = [part_ref[row] for row in range(rows)]
    latent[0] = latent[0] + from_low_ref[...]
    latent[rows - 1] = latent[rows - 1] + from_high_ref[...]
    stacked = to_tokens(latent, cols).astype(BF16)
    picked = jnp.dot(stacked, selection(lanes, cols), preferred_element_type=F32).astype(BF16)
    for y in range(2):
        for x in range(2):
            tokens_ref[(2 * y + x) * zc : (2 * y + x + 1) * zc] = picked[
                y * zc : (y + 1) * zc, x * lanes : (x + 1) * lanes
            ]


def prepare_kernel(bucket_ref, frames_ref, embed_ref, qgain_ref, kgain_ref, slot_ref, key_t_ref, qscale_ref, kscale_ref):
    seq = lax.axis_index("seq")
    me = lax.axis_index("group")
    src = [jnp.int32(0)] * CAP
    count = jnp.int32(0)
    for g in range(bucket_ref.shape[1]):
        hit = bucket_ref[seq, g] == me
        for slot in range(CAP):
            src[slot] = jnp.where(hit & (count == slot), g, src[slot])
        count = count + jnp.where(hit, 1, 0)
    for slot in range(CAP):
        slot_ref[0, slot] = src[slot]
        slot_ref[1, slot] = jnp.where(count > slot, frames_ref[seq, src[slot]], 0)
    key_t_ref[...] = jnp.transpose(embed_ref[:, D : 2 * D].astype(F32)).astype(BF16)
    qscale_ref[...] = qgain_ref[...] * math.log2(math.e)
    kscale_ref[...] = jnp.broadcast_to(column(kgain_ref[...]) * math.sqrt(HEAD), kscale_ref.shape)


def attend_kernel(slot_ref, *refs, sources, cols):
    token_refs = refs[:sources]
    embed_ref, key_t_ref, qscale_ref, kscale_ref, out_ref = refs[sources : 5 + sources]
    nat_scr, tr_scr, k_scr, q_scr, v_scr, p_scr, r_scr, out_scr, sem = refs[5 + sources :]
    me = lax.axis_index("group")
    tile = lax.axis_index("tile")
    tiles, _, lanes = token_refs[0].shape[-3:]
    frame_lane = lax.broadcasted_iota(jnp.int32, (1, lanes), 1) // cols
    frame_row = lax.broadcasted_iota(jnp.int32, (lanes, 1), 0) // cols
    counted, row_keep = [], []
    for slot in range(CAP):
        source = slot_ref[0, slot]
        total = slot_ref[1, slot]
        if sources == 1:
            raw = token_refs[0][source].astype(F32)
        else:
            raw = token_refs[0][...].astype(F32)
            for k in range(1, sources):
                raw = jnp.where((source ^ me) == k, token_refs[k][...].astype(F32), raw)
        valid = jnp.where(frame_lane < total, 1.0, 0.0)
        counted.append(jnp.where(frame_lane < jnp.maximum(total, 1), 1.0, 0.0))
        row_keep.append(jnp.where(frame_row < total, 1.0, 0.0))
        tokens_t = jnp.concatenate([raw[t] * valid for t in range(tiles)], axis=1)
        nat_scr[slot] = jnp.transpose(tokens_t).astype(BF16)
        tr_scr[slot] = tokens_t.astype(BF16)

    pairs = HEADS // 2
    steps = CAP * pairs

    def project(step):
        slot, pair = divmod(step, pairs)
        span = slice(pair * 2 * HEAD, (pair + 1) * 2 * HEAD)
        mine = nat_scr[slot, pl.ds(pl.multiple_of(tile * lanes, lanes), lanes), :]
        queries = jnp.dot(mine, embed_ref[:, span], preferred_element_type=F32)
        for half in range(2):
            one = slice(half * HEAD, (half + 1) * HEAD)
            k = jnp.dot(
                key_t_ref[span.start + one.start : span.start + one.stop, :],
                tr_scr[slot],
                preferred_element_type=F32,
            )
            k = k * lax.rsqrt(jnp.sum(k * k, axis=0, keepdims=True) + HEAD * EPS) * kscale_ref[...]
            k_scr[step % 2, half] = k.astype(BF16)
            q = queries[:, one]
            q = q * lax.rsqrt(jnp.sum(q * q, axis=1, keepdims=True) + HEAD * EPS) * qscale_ref[...]
            q_scr[step % 2, half] = q.astype(BF16)
        v_scr[step % 3] = jnp.dot(
            nat_scr[slot], embed_ref[:, 2 * D + span.start : 2 * D + span.stop], preferred_element_type=F32
        ).astype(BF16)

    def score(step):
        slot = step // pairs
        for half in range(2):
            scores = jnp.dot(q_scr[step % 2, half], k_scr[step % 2, half], preferred_element_type=F32)
            weights = jnp.exp2(scores)
            p_scr[step % 2, half] = weights.astype(BF16)
            folded = weights[:, :lanes]
            for t in range(1, tiles):
                folded = folded + weights[:, t * lanes : (t + 1) * lanes]
            totals = jnp.sum(folded * counted[slot], axis=1, keepdims=True)
            r_scr[step % 2, half] = row_keep[slot] / totals

    def mix(step):
        slot, pair = divmod(step, pairs)
        for half in range(2):
            one = slice(half * HEAD, (half + 1) * HEAD)
            mixed = jnp.dot(p_scr[step % 2, half], v_scr[step % 3, :, one], preferred_element_type=F32)
            start = pair * 2 * HEAD + one.start
            out_scr[slot, :, start : start + HEAD] = (mixed * r_scr[step % 2, half]).astype(BF16)

    copies = []
    for step in range(steps + 2):
        if step >= 2:
            mix(step - 2)
            if (step - 1) % pairs == 0:
                slot = (step - 2) // pairs
                copies.append(pltpu.make_async_copy(out_scr.at[slot], out_ref.at[slot], sem.at[slot]))
                copies[-1].start()
        if 1 <= step <= steps:
            score(step - 1)
        if step < steps:
            project(step)
    for copy in copies:
        copy.wait()


def clip_tokens(features, weight_t, bias_row):
    _, _, frames, rows, cols, channels = features.shape
    zc = bias_row.shape[1]
    lanes = frames * cols
    tiles = lax.axis_size("tile")
    scratch = [
        pltpu.VMEM((rows, frames, cols, channels), BF16),
        pltpu.VMEM(weight_t.shape, BF16),
        pltpu.VMEM(bias_row.shape, F32),
        pltpu.SemaphoreType.DMA((rows,)),
        pltpu.SemaphoreType.DMA,
        pltpu.SemaphoreType.DMA,
    ]
    if tiles == 2:
        send, keep = pl.pallas_call(
            conv_pair_kernel,
            out_shape=(pltpu.VMEM((rows + 3, zc, lanes), BF16), pltpu.VMEM((2, zc, lanes), F32)),
            in_specs=[HBM, HBM, HBM],
            out_specs=(VMEM, VMEM),
            scratch_shapes=scratch,
            name="conv",
        )(features, weight_t, bias_row)
        recv = lax.ppermute(send, "tile", [(0, 1), (1, 0)])
        return pl.pallas_call(
            functools.partial(finish_pair_kernel, cols=cols),
            out_shape=pltpu.VMEM((2, 4 * zc, lanes), BF16),
            in_specs=[VMEM, VMEM, VMEM],
            out_specs=VMEM,
            name="finish",
        )(*in_vmem(send, recv, keep))
    part, owed = pl.pallas_call(
        functools.partial(conv_any_kernel, tiles=tiles),
        out_shape=(pltpu.VMEM((rows, zc, lanes), F32), pltpu.VMEM((2, zc, lanes), F32)),
        in_specs=[HBM, HBM, HBM],
        out_specs=(VMEM, VMEM),
        scratch_shapes=scratch,
        name="conv",
    )(features, weight_t, bias_row)
    up = [(i, i + 1) for i in range(tiles - 1)]
    from_low = lax.ppermute(owed[0], "tile", up)
    from_high = lax.ppermute(owed[1], "tile", [(b, a) for a, b in up])
    tokens = pl.pallas_call(
        functools.partial(finish_any_kernel, cols=cols),
        out_shape=pltpu.VMEM((4 * zc, lanes), BF16),
        in_specs=[VMEM, VMEM, VMEM],
        out_specs=VMEM,
        name="finish",
    )(*in_vmem(part, from_low, from_high))
    return lax.all_gather(tokens, "tile", axis=0)


def shards(features, conv_weight, conv_bias, embed_qkv, query_gain, key_gain, bucket, frames):
    _, _, frame_count, rows, cols, channels = features.shape
    zc = conv_weight.shape[-1]
    lanes = frame_count * cols
    tiles = lax.axis_size("tile")
    groups = lax.axis_size("group")
    weight_t = jnp.transpose(conv_weight, (0, 1, 2, 4, 3)).reshape(-1, channels)
    tokens = clip_tokens(features, weight_t, conv_bias.reshape(1, -1))
    (embed,) = in_vmem(embed_qkv)
    slots, key_t, query_scale, key_scale = pl.pallas_call(
        prepare_kernel,
        out_shape=(
            pltpu.SMEM((2, CAP), jnp.int32),
            pltpu.VMEM((D, 4 * zc), BF16),
            pltpu.VMEM((1, HEAD), F32),
            pltpu.VMEM((HEAD, tiles * lanes), F32),
        ),
        in_specs=[SMEM, SMEM, VMEM, VMEM, VMEM],
        out_specs=(SMEM, VMEM, VMEM, VMEM),
        name="prepare",
    )(bucket, frames, embed, query_gain.reshape(1, -1), key_gain.reshape(1, -1))
    if groups in (2, 4):
        sources = [tokens] + [
            lax.ppermute(tokens, "group", [(i, i ^ k) for i in range(groups)]) for k in range(1, groups)
        ]
    else:
        sources = [lax.all_gather(tokens, "group", axis=0)]
    clip = tiles * lanes
    out = pl.pallas_call(
        functools.partial(attend_kernel, sources=len(sources), cols=cols),
        out_shape=jax.ShapeDtypeStruct((CAP, lanes, D), BF16),
        in_specs=[SMEM] + [VMEM] * (len(sources) + 4),
        out_specs=HBM,
        scratch_shapes=[
            pltpu.VMEM((CAP, clip, 4 * zc), BF16),
            pltpu.VMEM((CAP, 4 * zc, clip), BF16),
            pltpu.VMEM((2, 2, HEAD, clip), BF16),
            pltpu.VMEM((2, 2, lanes, HEAD), BF16),
            pltpu.VMEM((3, clip, 2 * HEAD), BF16),
            pltpu.VMEM((2, 2, lanes, clip), BF16),
            pltpu.VMEM((2, 2, lanes, 1), F32),
            pltpu.VMEM((CAP, lanes, D), BF16),
            pltpu.SemaphoreType.DMA((CAP,)),
        ],
        name="attend",
    )(pltpu.with_memory_space_constraint(slots, pltpu.SMEM), *in_vmem(*sources, embed, key_t, query_scale, key_scale))
    return out[None, None]


def solution(mesh):
    in_specs = (P("seq", "group", None, "tile", None, None), P(), P(), P(), P(), P(), P(), P())
    out_specs = P("seq", "group", None, "tile", None)
    return jax.shard_map(shards, mesh=mesh, in_specs=in_specs, out_specs=out_specs, check_vma=False)
```

```python
import functools
import math

import jax
import jax.numpy as jnp
from jax import lax
from jax.experimental import pallas as pl
from jax.experimental.pallas import tpu as pltpu
from jax.sharding import PartitionSpec as P

HEADS = 12
HEAD = 128
D = 1536
CAP = 2
EPS = 1e-06
BF16 = jnp.bfloat16
F32 = jnp.float32

VMEM = pl.BlockSpec(memory_space=pltpu.VMEM)
SMEM = pl.BlockSpec(memory_space=pltpu.SMEM)
HBM = pl.BlockSpec(memory_space=pltpu.HBM)


def in_vmem(*arrays):
    return [pltpu.with_memory_space_constraint(array, pltpu.VMEM) for array in arrays]


def column(row):
    size = row.shape[1]
    wide = jnp.broadcast_to(row, (size, size))
    down = lax.broadcasted_iota(jnp.int32, (size, size), 0)
    across = lax.broadcasted_iota(jnp.int32, (size, size), 1)
    return jnp.sum(jnp.where(down == across, wide, 0.0), axis=1, keepdims=True)


def conv_rows(features_ref, weight_ref, bias_ref, x_scr, w_scr, b_scr, x_sem, w_sem, b_sem, tiles):
    _, _, frames, rows, cols, _ = features_ref.shape
    lanes = frames * cols
    w_copy = pltpu.make_async_copy(weight_ref, w_scr, w_sem)
    w_copy.start()
    copies = []
    for row in range(rows):
        copy = pltpu.make_async_copy(features_ref.at[0, 0, :, row], x_scr.at[row], x_sem.at[row])
        copy.start()
        copies.append(copy)
    b_copy = pltpu.make_async_copy(bias_ref, b_scr, b_sem)
    b_copy.start()
    tile = lax.axis_index("tile")
    is_first = tile == 0
    is_last = tile == tiles - 1
    lane = lax.broadcasted_iota(jnp.int32, (16, lanes), 1)
    col = lane % cols
    in_first = lane < cols
    b_copy.wait()
    bias = column(b_scr[...])
    w_copy.wait()
    taps = []
    for pair in range(rows // 2):
        copies[2 * pair].wait()
        copies[2 * pair + 1].wait()
        block = x_scr[2 * pair : 2 * pair + 2].reshape(2 * lanes, -1)
        products = lax.dot_general(
            w_scr[...], block, (((1,), (1,)), ((), ())), preferred_element_type=F32
        )
        for half in range(2):
            part = products[:, half * lanes : (half + 1) * lanes]
            row_taps = []
            for b in range(3):
                row_taps.append([])
                for c in range(3):
                    tap = [part[(a * 9 + b * 3 + c) * 16 : (a * 9 + b * 3 + c + 1) * 16] for a in range(3)]
                    row_taps[b].append((tap[0] + tap[1], tap[2]))
            taps.append(row_taps)

    def finish(sums):
        def shifted(value, c):
            if c == 0:
                return jnp.where(col == 0, value, pltpu.roll(value, 1, 1))
            if c == 2:
                return jnp.where(col == cols - 1, value, pltpu.roll(value, lanes - 1, 1))
            return value

        early = sum(shifted(sums[c][0], c) for c in range(3))
        late = sum(shifted(sums[c][1], c) for c in range(3))
        return late + jnp.where(in_first, early, pltpu.roll(early, cols, 1))

    def add(*parts):
        return [tuple(sum(p[c][k] for p in parts) for k in range(2)) for c in range(3)]

    out = []
    for row in range(rows):
        parts = [taps[row + b - 1][b] for b in range(3) if 0 <= row + b - 1 < rows]
        value = finish(add(*parts)) + bias
        if row == 0:
            value = value + jnp.where(is_first, finish(taps[0][0]), 0.0)
        if row == rows - 1:
            value = value + jnp.where(is_last, finish(taps[rows - 1][2]), 0.0)
        out.append(value)
    return out, finish(taps[rows - 1][0]), finish(taps[0][2]), is_first


def conv_pair_kernel(features_ref, weight_ref, bias_ref, send_ref, keep_ref, *scratch):
    out, below, above, is_first = conv_rows(features_ref, weight_ref, bias_ref, *scratch, 2)
    rows = len(out)
    for row in range(rows):
        send_ref[row] = out[row].astype(BF16)
    edge = jnp.where(is_first, out[rows - 1], out[0])
    owed = jnp.where(is_first, below, above)
    keep_ref[0] = edge
    keep_ref[1] = owed
    send_ref[rows] = (edge - edge.astype(BF16).astype(F32)).astype(BF16)
    high = owed.astype(BF16)
    send_ref[rows + 1] = high
    send_ref[rows + 2] = (owed - high.astype(F32)).astype(BF16)


def selection(lanes, cols):
    shape = (2 * lanes, 2 * lanes)
    src = lax.broadcasted_iota(jnp.int32, shape, 0)
    dst = lax.broadcasted_iota(jnp.int32, shape, 1)
    half = cols // 2
    x = dst // lanes
    f = dst % lanes // cols
    i = dst % cols // half
    j = dst % half
    want = i * lanes + f * cols + 2 * j + x
    return jnp.where(src == want, 1.0, 0.0).astype(BF16)


def to_tokens(latent_rows, cols):
    blocks = [
        jnp.concatenate([latent_rows[y], latent_rows[2 + y]], axis=1) for y in range(2)
    ]
    return jnp.concatenate(blocks, axis=0)


def finish_pair_kernel(send_ref, recv_ref, keep_ref, tokens_ref, *, cols):
    is_first = lax.axis_index("tile") == 0
    slots, zc, lanes = send_ref.shape
    rows = slots - 3
    mine = [send_ref[row].astype(F32) for row in range(rows)]
    theirs = [recv_ref[row].astype(F32) for row in range(rows)]
    my_edge = keep_ref[0] + (recv_ref[rows + 1].astype(F32) + recv_ref[rows + 2].astype(F32))
    their_edge = jnp.where(is_first, theirs[0], theirs[rows - 1]) + recv_ref[rows].astype(F32) + keep_ref[1]
    mine[0] = jnp.where(is_first, mine[0], my_edge)
    mine[rows - 1] = jnp.where(is_first, my_edge, mine[rows - 1])
    theirs[0] = jnp.where(is_first, their_edge, theirs[0])
    theirs[rows - 1] = jnp.where(is_first, theirs[rows - 1], their_edge)
    low = [jnp.where(is_first, a, b) for a, b in zip(mine, theirs)]
    high = [jnp.where(is_first, b, a) for a, b in zip(mine, theirs)]
    stacked = jnp.concatenate([to_tokens(low, cols), to_tokens(high, cols)], axis=0).astype(BF16)
    picked = jnp.dot(stacked, selection(lanes, cols), preferred_element_type=F32).astype(BF16)
    for t in range(2):
        for y in range(2):
            for x in range(2):
                tokens_ref[t, (2 * y + x) * zc : (2 * y + x + 1) * zc] = picked[
                    (2 * t + y) * zc : (2 * t + y + 1) * zc, x * lanes : (x + 1) * lanes
                ]


def conv_any_kernel(features_ref, weight_ref, bias_ref, part_ref, owed_ref, *scratch, tiles):
    out, below, above, _ = conv_rows(features_ref, weight_ref, bias_ref, *scratch, tiles)
    for row, value in enumerate(out):
        part_ref[row] = value
    owed_ref[0] = below
    owed_ref[1] = above


def finish_any_kernel(part_ref, from_low_ref, from_high_ref, tokens_ref, *, cols):
    rows, zc, lanes = part_ref.shape
    latent = [part_ref[row] for row in range(rows)]
    latent[0] = latent[0] + from_low_ref[...]
    latent[rows - 1] = latent[rows - 1] + from_high_ref[...]
    stacked = to_tokens(latent, cols).astype(BF16)
    picked = jnp.dot(stacked, selection(lanes, cols), preferred_element_type=F32).astype(BF16)
    for y in range(2):
        for x in range(2):
            tokens_ref[(2 * y + x) * zc : (2 * y + x + 1) * zc] = picked[
                y * zc : (y + 1) * zc, x * lanes : (x + 1) * lanes
            ]


def prepare_kernel(bucket_ref, frames_ref, embed_ref, qgain_ref, kgain_ref, slot_ref, key_t_ref, qscale_ref, kscale_ref):
    seq = lax.axis_index("seq")
    me = lax.axis_index("group")
    src = [jnp.int32(0)] * CAP
    count = jnp.int32(0)
    for g in range(bucket_ref.shape[1]):
        hit = bucket_ref[seq, g] == me
        for slot in range(CAP):
            src[slot] = jnp.where(hit & (count == slot), g, src[slot])
        count = count + jnp.where(hit, 1, 0)
    for slot in range(CAP):
        slot_ref[0, slot] = src[slot]
        slot_ref[1, slot] = jnp.where(count > slot, frames_ref[seq, src[slot]], 0)
    key_t_ref[...] = jnp.transpose(embed_ref[:, D : 2 * D].astype(F32)).astype(BF16)
    qscale_ref[...] = qgain_ref[...] * math.log2(math.e)
    kscale_ref[...] = jnp.broadcast_to(column(kgain_ref[...]) * math.sqrt(HEAD), kscale_ref.shape)


def attend_kernel(slot_ref, *refs, sources, cols):
    token_refs = refs[:sources]
    embed_ref, key_t_ref, qscale_ref, kscale_ref, out_ref = refs[sources : 5 + sources]
    nat_scr, tr_scr, k_scr, q_scr, v_scr, p_scr, r_scr, out_scr, sem = refs[5 + sources :]
    me = lax.axis_index("group")
    tile = lax.axis_index("tile")
    tiles, _, lanes = token_refs[0].shape[-3:]
    frame_lane = lax.broadcasted_iota(jnp.int32, (1, lanes), 1) // cols
    frame_row = lax.broadcasted_iota(jnp.int32, (lanes, 1), 0) // cols
    counted, row_keep = [], []
    for slot in range(CAP):
        source = slot_ref[0, slot]
        total = slot_ref[1, slot]
        if sources == 1:
            raw = token_refs[0][source].astype(F32)
        else:
            raw = token_refs[0][...].astype(F32)
            for k in range(1, sources):
                raw = jnp.where((source ^ me) == k, token_refs[k][...].astype(F32), raw)
        valid = jnp.where(frame_lane < total, 1.0, 0.0)
        counted.append(jnp.where(frame_lane < jnp.maximum(total, 1), 1.0, 0.0))
        row_keep.append(jnp.where(frame_row < total, 1.0, 0.0))
        tokens_t = jnp.concatenate([raw[t] * valid for t in range(tiles)], axis=1)
        nat_scr[slot] = jnp.transpose(tokens_t).astype(BF16)
        tr_scr[slot] = tokens_t.astype(BF16)

    pairs = HEADS // 2
    steps = CAP * pairs

    def project_k(step, half):
        slot, pair = divmod(step, pairs)
        start = (2 * pair + half) * HEAD
        k = jnp.dot(key_t_ref[start : start + HEAD, :], tr_scr[slot], preferred_element_type=F32)
        k = k * lax.rsqrt(jnp.sum(k * k, axis=0, keepdims=True) + HEAD * EPS) * kscale_ref[...]
        k_scr[step % 2, half] = k.astype(BF16)

    def project_q(step):
        slot, pair = divmod(step, pairs)
        span = slice(pair * 2 * HEAD, (pair + 1) * 2 * HEAD)
        mine = nat_scr[slot, pl.ds(pl.multiple_of(tile * lanes, lanes), lanes), :]
        queries = jnp.dot(mine, embed_ref[:, span], preferred_element_type=F32)
        for half in range(2):
            q = queries[:, half * HEAD : (half + 1) * HEAD]
            q = q * lax.rsqrt(jnp.sum(q * q, axis=1, keepdims=True) + HEAD * EPS) * qscale_ref[...]
            q_scr[step % 2, half] = q.astype(BF16)

    def project_v(step):
        slot, pair = divmod(step, pairs)
        start = 2 * D + pair * 2 * HEAD
        v_scr[step % 3] = jnp.dot(
            nat_scr[slot], embed_ref[:, start : start + 2 * HEAD], preferred_element_type=F32
        ).astype(BF16)

    def score(step, half):
        slot = step // pairs
        scores = jnp.dot(q_scr[step % 2, half], k_scr[step % 2, half], preferred_element_type=F32)
        weights = jnp.exp2(scores)
        p_scr[step % 2, half] = weights.astype(BF16)
        folded = weights[:, :lanes]
        for t in range(1, tiles):
            folded = folded + weights[:, t * lanes : (t + 1) * lanes]
        totals = jnp.sum(folded * counted[slot], axis=1, keepdims=True)
        r_scr[step % 2, half] = jnp.broadcast_to(row_keep[slot] / totals, (lanes, HEAD))

    def mix(step, half):
        slot, pair = divmod(step, pairs)
        start = (2 * pair + half) * HEAD
        mixed = jnp.dot(
            p_scr[step % 2, half], v_scr[step % 3, :, half * HEAD : (half + 1) * HEAD], preferred_element_type=F32
        )
        out_scr[slot, :, start : start + HEAD] = (mixed * r_scr[step % 2, half]).astype(BF16)
        if half == 1:
            part = (slot, slice(None), pl.ds(pair * 2 * HEAD, 2 * HEAD))
            copies.append(pltpu.make_async_copy(out_scr.at[part], out_ref.at[part], sem.at[step]))
            copies[-1].start()

    copies = []
    for step in range(steps + 2):
        here, last, before = step < steps, 1 <= step <= steps, step >= 2
        if here:
            project_q(step)
        if here:
            project_k(step, 0)
        if here:
            project_k(step, 1)
        if here:
            project_v(step)
        if last:
            score(step - 1, 0)
        if last:
            score(step - 1, 1)
        if before:
            mix(step - 2, 0)
        if before:
            mix(step - 2, 1)
    for copy in copies:
        copy.wait()


def clip_tokens(features, weight_t, bias_row):
    _, _, frames, rows, cols, channels = features.shape
    zc = bias_row.shape[1]
    lanes = frames * cols
    tiles = lax.axis_size("tile")
    scratch = [
        pltpu.VMEM((rows, frames, cols, channels), BF16),
        pltpu.VMEM(weight_t.shape, BF16),
        pltpu.VMEM(bias_row.shape, F32),
        pltpu.SemaphoreType.DMA((rows,)),
        pltpu.SemaphoreType.DMA,
        pltpu.SemaphoreType.DMA,
    ]
    if tiles == 2:
        send, keep = pl.pallas_call(
            conv_pair_kernel,
            out_shape=(pltpu.VMEM((rows + 3, zc, lanes), BF16), pltpu.VMEM((2, zc, lanes), F32)),
            in_specs=[HBM, HBM, HBM],
            out_specs=(VMEM, VMEM),
            scratch_shapes=scratch,
            name="conv",
        )(features, weight_t, bias_row)
        recv = lax.ppermute(send, "tile", [(0, 1), (1, 0)])
        return pl.pallas_call(
            functools.partial(finish_pair_kernel, cols=cols),
            out_shape=pltpu.VMEM((2, 4 * zc, lanes), BF16),
            in_specs=[VMEM, VMEM, VMEM],
            out_specs=VMEM,
            name="finish",
        )(*in_vmem(send, recv, keep))
    part, owed = pl.pallas_call(
        functools.partial(conv_any_kernel, tiles=tiles),
        out_shape=(pltpu.VMEM((rows, zc, lanes), F32), pltpu.VMEM((2, zc, lanes), F32)),
        in_specs=[HBM, HBM, HBM],
        out_specs=(VMEM, VMEM),
        scratch_shapes=scratch,
        name="conv",
    )(features, weight_t, bias_row)
    up = [(i, i + 1) for i in range(tiles - 1)]
    from_low = lax.ppermute(owed[0], "tile", up)
    from_high = lax.ppermute(owed[1], "tile", [(b, a) for a, b in up])
    tokens = pl.pallas_call(
        functools.partial(finish_any_kernel, cols=cols),
        out_shape=pltpu.VMEM((4 * zc, lanes), BF16),
        in_specs=[VMEM, VMEM, VMEM],
        out_specs=VMEM,
        name="finish",
    )(*in_vmem(part, from_low, from_high))
    return lax.all_gather(tokens, "tile", axis=0)


def shards(features, conv_weight, conv_bias, embed_qkv, query_gain, key_gain, bucket, frames):
    _, _, frame_count, rows, cols, channels = features.shape
    zc = conv_weight.shape[-1]
    lanes = frame_count * cols
    tiles = lax.axis_size("tile")
    groups = lax.axis_size("group")
    weight_t = jnp.transpose(conv_weight, (0, 1, 2, 4, 3)).reshape(-1, channels)
    tokens = clip_tokens(features, weight_t, conv_bias.reshape(1, -1))
    (embed,) = in_vmem(embed_qkv)
    slots, key_t, query_scale, key_scale = pl.pallas_call(
        prepare_kernel,
        out_shape=(
            pltpu.SMEM((2, CAP), jnp.int32),
            pltpu.VMEM((D, 4 * zc), BF16),
            pltpu.VMEM((1, HEAD), F32),
            pltpu.VMEM((HEAD, tiles * lanes), F32),
        ),
        in_specs=[SMEM, SMEM, VMEM, VMEM, VMEM],
        out_specs=(SMEM, VMEM, VMEM, VMEM),
        name="prepare",
    )(bucket, frames, embed, query_gain.reshape(1, -1), key_gain.reshape(1, -1))
    if groups in (2, 4):
        sources = [tokens] + [
            lax.ppermute(tokens, "group", [(i, i ^ k) for i in range(groups)]) for k in range(1, groups)
        ]
    else:
        sources = [lax.all_gather(tokens, "group", axis=0)]
    clip = tiles * lanes
    out = pl.pallas_call(
        functools.partial(attend_kernel, sources=len(sources), cols=cols),
        out_shape=jax.ShapeDtypeStruct((CAP, lanes, D), BF16),
        in_specs=[SMEM] + [VMEM] * (len(sources) + 4),
        out_specs=HBM,
        scratch_shapes=[
            pltpu.VMEM((CAP, clip, 4 * zc), BF16),
            pltpu.VMEM((CAP, 4 * zc, clip), BF16),
            pltpu.VMEM((2, 2, HEAD, clip), BF16),
            pltpu.VMEM((2, 2, lanes, HEAD), BF16),
            pltpu.VMEM((3, clip, 2 * HEAD), BF16),
            pltpu.VMEM((2, 2, lanes, clip), BF16),
            pltpu.VMEM((2, 2, lanes, HEAD), F32),
            pltpu.VMEM((CAP, lanes, D), BF16),
            pltpu.SemaphoreType.DMA((CAP * HEADS // 2,)),
        ],
        name="attend",
    )(pltpu.with_memory_space_constraint(slots, pltpu.SMEM), *in_vmem(*sources, embed, key_t, query_scale, key_scale))
    return out[None, None]


def solution(mesh):
    in_specs = (P("seq", "group", None, "tile", None, None), P(), P(), P(), P(), P(), P(), P())
    out_specs = P("seq", "group", None, "tile", None)
    return jax.shard_map(shards, mesh=mesh, in_specs=in_specs, out_specs=out_specs, check_vma=False)
```

```python
import functools
import math

import jax
import jax.numpy as jnp
from jax import lax
from jax.experimental import pallas as pl
from jax.experimental.pallas import tpu as pltpu
from jax.sharding import PartitionSpec as P

HEADS = 12
HEAD = 128
D = 1536
CAP = 2
EPS = 1e-06
BF16 = jnp.bfloat16
F32 = jnp.float32

VMEM = pl.BlockSpec(memory_space=pltpu.VMEM)
SMEM = pl.BlockSpec(memory_space=pltpu.SMEM)
HBM = pl.BlockSpec(memory_space=pltpu.HBM)


def in_vmem(*arrays):
    return [pltpu.with_memory_space_constraint(array, pltpu.VMEM) for array in arrays]


def column(row):
    size = row.shape[1]
    wide = jnp.broadcast_to(row, (size, size))
    down = lax.broadcasted_iota(jnp.int32, (size, size), 0)
    across = lax.broadcasted_iota(jnp.int32, (size, size), 1)
    return jnp.sum(jnp.where(down == across, wide, 0.0), axis=1, keepdims=True)


def conv_rows(features_ref, weight_ref, bias_ref, x_scr, w_scr, b_scr, x_sem, w_sem, b_sem, tiles):
    _, _, frames, rows, cols, _ = features_ref.shape
    lanes = frames * cols
    w_copy = pltpu.make_async_copy(weight_ref, w_scr, w_sem)
    w_copy.start()
    copies = []
    for row in range(rows):
        copy = pltpu.make_async_copy(features_ref.at[0, 0, :, row], x_scr.at[row], x_sem.at[row])
        copy.start()
        copies.append(copy)
    b_copy = pltpu.make_async_copy(bias_ref, b_scr, b_sem)
    b_copy.start()
    tile = lax.axis_index("tile")
    is_first = tile == 0
    is_last = tile == tiles - 1
    lane = lax.broadcasted_iota(jnp.int32, (16, lanes), 1)
    col = lane % cols
    in_first = lane < cols
    b_copy.wait()
    bias = column(b_scr[...])
    w_copy.wait()
    taps = []
    for pair in range(rows // 2):
        copies[2 * pair].wait()
        copies[2 * pair + 1].wait()
        block = x_scr[2 * pair : 2 * pair + 2].reshape(2 * lanes, -1)
        products = lax.dot_general(
            w_scr[...], block, (((1,), (1,)), ((), ())), preferred_element_type=F32
        )
        for half in range(2):
            part = products[:, half * lanes : (half + 1) * lanes]
            row_taps = []
            for b in range(3):
                row_taps.append([])
                for c in range(3):
                    tap = [part[(a * 9 + b * 3 + c) * 16 : (a * 9 + b * 3 + c + 1) * 16] for a in range(3)]
                    row_taps[b].append((tap[0] + tap[1], tap[2]))
            taps.append(row_taps)

    def finish(sums):
        def shifted(value, c):
            if c == 0:
                return jnp.where(col == 0, value, pltpu.roll(value, 1, 1))
            if c == 2:
                return jnp.where(col == cols - 1, value, pltpu.roll(value, lanes - 1, 1))
            return value

        early = sum(shifted(sums[c][0], c) for c in range(3))
        late = sum(shifted(sums[c][1], c) for c in range(3))
        return late + jnp.where(in_first, early, pltpu.roll(early, cols, 1))

    def add(*parts):
        return [tuple(sum(p[c][k] for p in parts) for k in range(2)) for c in range(3)]

    def where(flag, one, other):
        return [
            tuple(jnp.where(flag, one[c][k], 0.0 if other is None else other[c][k]) for k in range(2))
            for c in range(3)
        ]

    out = []
    for row in range(rows):
        parts = [taps[row + b - 1][b] for b in range(3) if 0 <= row + b - 1 < rows]
        if row == 0:
            parts.append(where(is_first, taps[0][0], None))
        if row == rows - 1:
            parts.append(where(is_last, taps[rows - 1][2], None))
        out.append(finish(add(*parts)) + bias)
    if tiles == 2:
        return out, (finish(where(is_first, taps[rows - 1][0], taps[0][2])),), is_first
    return out, (finish(taps[rows - 1][0]), finish(taps[0][2])), is_first


def conv_pair_kernel(features_ref, weight_ref, bias_ref, send_ref, keep_ref, *scratch):
    out, (owed,), is_first = conv_rows(features_ref, weight_ref, bias_ref, *scratch, 2)
    rows = len(out)
    for row in range(rows):
        send_ref[row] = out[row].astype(BF16)
    edge = jnp.where(is_first, out[rows - 1], out[0])
    keep_ref[0] = edge
    keep_ref[1] = owed
    send_ref[rows] = (edge - edge.astype(BF16).astype(F32)).astype(BF16)
    high = owed.astype(BF16)
    send_ref[rows + 1] = high
    send_ref[rows + 2] = (owed - high.astype(F32)).astype(BF16)


def selection(lanes, cols):
    shape = (2 * lanes, 2 * lanes)
    src = lax.broadcasted_iota(jnp.int32, shape, 0)
    dst = lax.broadcasted_iota(jnp.int32, shape, 1)
    half = cols // 2
    x = dst // lanes
    f = dst % lanes // cols
    i = dst % cols // half
    j = dst % half
    want = i * lanes + f * cols + 2 * j + x
    return jnp.where(src == want, 1.0, 0.0).astype(BF16)


def to_tokens(latent_rows, cols):
    blocks = [
        jnp.concatenate([latent_rows[y], latent_rows[2 + y]], axis=1) for y in range(2)
    ]
    return jnp.concatenate(blocks, axis=0)


def finish_pair_kernel(send_ref, recv_ref, keep_ref, tokens_ref, *, cols):
    is_first = lax.axis_index("tile") == 0
    slots, zc, lanes = send_ref.shape
    rows = slots - 3
    mine = [send_ref[row].astype(F32) for row in range(rows)]
    theirs = [recv_ref[row].astype(F32) for row in range(rows)]
    my_edge = keep_ref[0] + (recv_ref[rows + 1].astype(F32) + recv_ref[rows + 2].astype(F32))
    their_edge = jnp.where(is_first, theirs[0], theirs[rows - 1]) + recv_ref[rows].astype(F32) + keep_ref[1]
    mine[0] = jnp.where(is_first, mine[0], my_edge)
    mine[rows - 1] = jnp.where(is_first, my_edge, mine[rows - 1])
    theirs[0] = jnp.where(is_first, their_edge, theirs[0])
    theirs[rows - 1] = jnp.where(is_first, theirs[rows - 1], their_edge)
    low = [jnp.where(is_first, a, b) for a, b in zip(mine, theirs)]
    high = [jnp.where(is_first, b, a) for a, b in zip(mine, theirs)]
    stacked = jnp.concatenate([to_tokens(low, cols), to_tokens(high, cols)], axis=0).astype(BF16)
    picked = jnp.dot(stacked, selection(lanes, cols), preferred_element_type=F32).astype(BF16)
    for t in range(2):
        for y in range(2):
            for x in range(2):
                tokens_ref[t, (2 * y + x) * zc : (2 * y + x + 1) * zc] = picked[
                    (2 * t + y) * zc : (2 * t + y + 1) * zc, x * lanes : (x + 1) * lanes
                ]


def conv_any_kernel(features_ref, weight_ref, bias_ref, part_ref, owed_ref, *scratch, tiles):
    out, owed, _ = conv_rows(features_ref, weight_ref, bias_ref, *scratch, tiles)
    for row, value in enumerate(out):
        part_ref[row] = value
    owed_ref[0] = owed[0]
    owed_ref[1] = owed[1]


def finish_any_kernel(part_ref, from_low_ref, from_high_ref, tokens_ref, *, cols):
    rows, zc, lanes = part_ref.shape
    latent = [part_ref[row] for row in range(rows)]
    latent[0] = latent[0] + from_low_ref[...]
    latent[rows - 1] = latent[rows - 1] + from_high_ref[...]
    stacked = to_tokens(latent, cols).astype(BF16)
    picked = jnp.dot(stacked, selection(lanes, cols), preferred_element_type=F32).astype(BF16)
    for y in range(2):
        for x in range(2):
            tokens_ref[(2 * y + x) * zc : (2 * y + x + 1) * zc] = picked[
                y * zc : (y + 1) * zc, x * lanes : (x + 1) * lanes
            ]


def prepare_kernel(bucket_ref, frames_ref, embed_ref, qgain_ref, kgain_ref, slot_ref, key_t_ref, qscale_ref, kscale_ref):
    seq = lax.axis_index("seq")
    me = lax.axis_index("group")
    src = [jnp.int32(0)] * CAP
    count = jnp.int32(0)
    for g in range(bucket_ref.shape[1]):
        hit = bucket_ref[seq, g] == me
        for slot in range(CAP):
            src[slot] = jnp.where(hit & (count == slot), g, src[slot])
        count = count + jnp.where(hit, 1, 0)
    for slot in range(CAP):
        slot_ref[0, slot] = src[slot]
        slot_ref[1, slot] = jnp.where(count > slot, frames_ref[seq, src[slot]], 0)
    key_t_ref[...] = jnp.transpose(embed_ref[:, D : 2 * D].astype(F32)).astype(BF16)
    qscale_ref[...] = qgain_ref[...] * math.log2(math.e)
    kscale_ref[...] = jnp.broadcast_to(column(kgain_ref[...]) * math.sqrt(HEAD), kscale_ref.shape)


def attend_kernel(slot_ref, *refs, sources, cols):
    token_refs = refs[:sources]
    embed_ref, key_t_ref, qscale_ref, kscale_ref, out_ref = refs[sources : 5 + sources]
    nat_scr, tr_scr, k_scr, q_scr, v_scr, p_scr, r_scr, out_scr, sem = refs[5 + sources :]
    me = lax.axis_index("group")
    tile = lax.axis_index("tile")
    tiles, _, lanes = token_refs[0].shape[-3:]
    frame_lane = lax.broadcasted_iota(jnp.int32, (1, lanes), 1) // cols
    frame_row = lax.broadcasted_iota(jnp.int32, (lanes, 1), 0) // cols
    counted, row_keep = [], []
    for slot in range(CAP):
        source = slot_ref[0, slot]
        total = slot_ref[1, slot]
        if sources == 1:
            raw = token_refs[0][source].astype(F32)
        else:
            raw = token_refs[0][...].astype(F32)
            for k in range(1, sources):
                raw = jnp.where((source ^ me) == k, token_refs[k][...].astype(F32), raw)
        valid = jnp.where(frame_lane < total, 1.0, 0.0)
        counted.append(jnp.where(frame_lane < jnp.maximum(total, 1), 1.0, 0.0))
        row_keep.append(jnp.where(frame_row < total, 1.0, 0.0))
        tokens_t = jnp.concatenate([raw[t] * valid for t in range(tiles)], axis=1)
        nat_scr[slot] = jnp.transpose(tokens_t).astype(BF16)
        tr_scr[slot] = tokens_t.astype(BF16)

    pairs = HEADS // 2

    def project_k(step, half):
        slot, pair = divmod(step, pairs)
        start = (2 * pair + half) * HEAD
        k = jnp.dot(key_t_ref[start : start + HEAD, :], tr_scr[slot], preferred_element_type=F32)
        k = k * lax.rsqrt(jnp.sum(k * k, axis=0, keepdims=True) + HEAD * EPS) * kscale_ref[...]
        k_scr[step % 2, half] = k.astype(BF16)

    def project_q(step):
        slot, pair = divmod(step, pairs)
        span = slice(pair * 2 * HEAD, (pair + 1) * 2 * HEAD)
        mine = nat_scr[slot, pl.ds(pl.multiple_of(tile * lanes, lanes), lanes), :]
        queries = jnp.dot(mine, embed_ref[:, span], preferred_element_type=F32)
        for half in range(2):
            q = queries[:, half * HEAD : (half + 1) * HEAD]
            q = q * lax.rsqrt(jnp.sum(q * q, axis=1, keepdims=True) + HEAD * EPS) * qscale_ref[...]
            q_scr[step % 2, half] = q.astype(BF16)

    def project_v(step):
        slot, pair = divmod(step, pairs)
        start = 2 * D + pair * 2 * HEAD
        v_scr[step % 3] = jnp.dot(
            nat_scr[slot], embed_ref[:, start : start + 2 * HEAD], preferred_element_type=F32
        ).astype(BF16)

    def score(step, half):
        slot = step // pairs
        scores = jnp.dot(q_scr[step % 2, half], k_scr[step % 2, half], preferred_element_type=F32)
        weights = jnp.exp2(scores)
        p_scr[step % 2, half] = weights.astype(BF16)
        folded = weights[:, :lanes]
        for t in range(1, tiles):
            folded = folded + weights[:, t * lanes : (t + 1) * lanes]
        totals = jnp.sum(folded * counted[slot], axis=1, keepdims=True)
        r_scr[step % 2, half] = jnp.broadcast_to(row_keep[slot] / totals, (lanes, HEAD))

    def mix(step, half):
        slot, pair = divmod(step, pairs)
        start = (2 * pair + half) * HEAD
        mixed = jnp.dot(
            p_scr[step % 2, half], v_scr[step % 3, :, half * HEAD : (half + 1) * HEAD], preferred_element_type=F32
        )
        out_scr[slot, :, start : start + HEAD] = (mixed * r_scr[step % 2, half]).astype(BF16)
        if half == 1:
            part = (slot, slice(None), pl.ds(pair * 2 * HEAD, 2 * HEAD))
            copies.append(pltpu.make_async_copy(out_scr.at[part], out_ref.at[part], sem.at[step]))
            copies[-1].start()

    copies = []

    def run(slots):
        steps = slots * pairs
        for slot in range(slots, CAP):
            out_scr[slot] = jnp.zeros(out_scr.shape[1:], BF16)
            copies.append(pltpu.make_async_copy(out_scr.at[slot], out_ref.at[slot], sem.at[slot * pairs]))
            copies[-1].start()
        for step in range(steps + 2):
            here, last, before = step < steps, 1 <= step <= steps, step >= 2
            if here:
                project_q(step)
                project_k(step, 0)
                project_k(step, 1)
                project_v(step)
            if last:
                score(step - 1, 0)
                score(step - 1, 1)
            if before:
                mix(step - 2, 0)
                mix(step - 2, 1)
        for copy in copies:
            copy.wait()
        copies.clear()

    double = slot_ref[1, CAP - 1] > 0

    @pl.when(double)
    def _():
        run(CAP)

    @pl.when(jnp.logical_not(double))
    def _():
        run(1)


def clip_tokens(features, weight_t, bias_row):
    _, _, frames, rows, cols, channels = features.shape
    zc = bias_row.shape[1]
    lanes = frames * cols
    tiles = lax.axis_size("tile")
    scratch = [
        pltpu.VMEM((rows, frames, cols, channels), BF16),
        pltpu.VMEM(weight_t.shape, BF16),
        pltpu.VMEM(bias_row.shape, F32),
        pltpu.SemaphoreType.DMA((rows,)),
        pltpu.SemaphoreType.DMA,
        pltpu.SemaphoreType.DMA,
    ]
    if tiles == 2:
        send, keep = pl.pallas_call(
            conv_pair_kernel,
            out_shape=(pltpu.VMEM((rows + 3, zc, lanes), BF16), pltpu.VMEM((2, zc, lanes), F32)),
            in_specs=[HBM, HBM, HBM],
            out_specs=(VMEM, VMEM),
            scratch_shapes=scratch,
            name="conv",
        )(features, weight_t, bias_row)
        recv = lax.ppermute(send, "tile", [(0, 1), (1, 0)])
        return pl.pallas_call(
            functools.partial(finish_pair_kernel, cols=cols),
            out_shape=pltpu.VMEM((2, 4 * zc, lanes), BF16),
            in_specs=[VMEM, VMEM, VMEM],
            out_specs=VMEM,
            name="finish",
        )(*in_vmem(send, recv, keep))
    part, owed = pl.pallas_call(
        functools.partial(conv_any_kernel, tiles=tiles),
        out_shape=(pltpu.VMEM((rows, zc, lanes), F32), pltpu.VMEM((2, zc, lanes), F32)),
        in_specs=[HBM, HBM, HBM],
        out_specs=(VMEM, VMEM),
        scratch_shapes=scratch,
        name="conv",
    )(features, weight_t, bias_row)
    up = [(i, i + 1) for i in range(tiles - 1)]
    from_low = lax.ppermute(owed[0], "tile", up)
    from_high = lax.ppermute(owed[1], "tile", [(b, a) for a, b in up])
    tokens = pl.pallas_call(
        functools.partial(finish_any_kernel, cols=cols),
        out_shape=pltpu.VMEM((4 * zc, lanes), BF16),
        in_specs=[VMEM, VMEM, VMEM],
        out_specs=VMEM,
        name="finish",
    )(*in_vmem(part, from_low, from_high))
    return lax.all_gather(tokens, "tile", axis=0)


def shards(features, conv_weight, conv_bias, embed_qkv, query_gain, key_gain, bucket, frames):
    _, _, frame_count, rows, cols, channels = features.shape
    zc = conv_weight.shape[-1]
    lanes = frame_count * cols
    tiles = lax.axis_size("tile")
    groups = lax.axis_size("group")
    weight_t = jnp.transpose(conv_weight, (0, 1, 2, 4, 3)).reshape(-1, channels)
    tokens = clip_tokens(features, weight_t, conv_bias.reshape(1, -1))
    (embed,) = in_vmem(embed_qkv)
    slots, key_t, query_scale, key_scale = pl.pallas_call(
        prepare_kernel,
        out_shape=(
            pltpu.SMEM((2, CAP), jnp.int32),
            pltpu.VMEM((D, 4 * zc), BF16),
            pltpu.VMEM((1, HEAD), F32),
            pltpu.VMEM((HEAD, tiles * lanes), F32),
        ),
        in_specs=[SMEM, SMEM, VMEM, VMEM, VMEM],
        out_specs=(SMEM, VMEM, VMEM, VMEM),
        name="prepare",
    )(bucket, frames, embed, query_gain.reshape(1, -1), key_gain.reshape(1, -1))
    if groups in (2, 4):
        sources = [tokens] + [
            lax.ppermute(tokens, "group", [(i, i ^ k) for i in range(groups)]) for k in range(1, groups)
        ]
    else:
        sources = [lax.all_gather(tokens, "group", axis=0)]
    clip = tiles * lanes
    out = pl.pallas_call(
        functools.partial(attend_kernel, sources=len(sources), cols=cols),
        out_shape=jax.ShapeDtypeStruct((CAP, lanes, D), BF16),
        in_specs=[SMEM] + [VMEM] * (len(sources) + 4),
        out_specs=HBM,
        scratch_shapes=[
            pltpu.VMEM((CAP, clip, 4 * zc), BF16),
            pltpu.VMEM((CAP, 4 * zc, clip), BF16),
            pltpu.VMEM((2, 2, HEAD, clip), BF16),
            pltpu.VMEM((2, 2, lanes, HEAD), BF16),
            pltpu.VMEM((3, clip, 2 * HEAD), BF16),
            pltpu.VMEM((2, 2, lanes, clip), BF16),
            pltpu.VMEM((2, 2, lanes, HEAD), F32),
            pltpu.VMEM((CAP, lanes, D), BF16),
            pltpu.SemaphoreType.DMA((CAP * HEADS // 2,)),
        ],
        name="attend",
    )(pltpu.with_memory_space_constraint(slots, pltpu.SMEM), *in_vmem(*sources, embed, key_t, query_scale, key_scale))
    return out[None, None]


def solution(mesh):
    in_specs = (P("seq", "group", None, "tile", None, None), P(), P(), P(), P(), P(), P(), P())
    out_specs = P("seq", "group", None, "tile", None)
    return jax.shard_map(shards, mesh=mesh, in_specs=in_specs, out_specs=out_specs, check_vma=False)
```

```python
import functools
import math

import jax
import jax.numpy as jnp
from jax import lax
from jax.experimental import pallas as pl
from jax.experimental.pallas import tpu as pltpu
from jax.sharding import PartitionSpec as P

HEADS = 12
HEAD = 128
D = 1536
CAP = 2
EPS = 1e-06
BF16 = jnp.bfloat16
F32 = jnp.float32

VMEM = pl.BlockSpec(memory_space=pltpu.VMEM)
SMEM = pl.BlockSpec(memory_space=pltpu.SMEM)
HBM = pl.BlockSpec(memory_space=pltpu.HBM)


def in_vmem(*arrays):
    return [pltpu.with_memory_space_constraint(array, pltpu.VMEM) for array in arrays]


def column(row):
    size = row.shape[1]
    wide = jnp.broadcast_to(row, (size, size))
    down = lax.broadcasted_iota(jnp.int32, (size, size), 0)
    across = lax.broadcasted_iota(jnp.int32, (size, size), 1)
    return jnp.sum(jnp.where(down == across, wide, 0.0), axis=1, keepdims=True)


def conv_rows(features_ref, weight_ref, bias_ref, x_scr, w_scr, b_scr, x_sem, w_sem, b_sem, tiles):
    _, _, frames, rows, cols, _ = features_ref.shape
    lanes = frames * cols
    w_copy = pltpu.make_async_copy(weight_ref, w_scr, w_sem)
    w_copy.start()
    copies = []
    for row in range(rows):
        copy = pltpu.make_async_copy(features_ref.at[0, 0, :, row], x_scr.at[row], x_sem.at[row])
        copy.start()
        copies.append(copy)
    b_copy = pltpu.make_async_copy(bias_ref, b_scr, b_sem)
    b_copy.start()
    tile = lax.axis_index("tile")
    is_first = tile == 0
    is_last = tile == tiles - 1
    lane = lax.broadcasted_iota(jnp.int32, (16, lanes), 1)
    col = lane % cols
    in_first = lane < cols
    b_copy.wait()
    bias = column(b_scr[...])
    w_copy.wait()
    for copy in copies:
        copy.wait()
    taps = []
    for pair in range(rows // 2):
        block = x_scr[2 * pair : 2 * pair + 2].reshape(2 * lanes, -1)
        products = lax.dot_general(
            w_scr[...], block, (((1,), (1,)), ((), ())), preferred_element_type=F32
        )
        for half in range(2):
            part = products[:, half * lanes : (half + 1) * lanes]
            row_taps = []
            for b in range(3):
                row_taps.append([])
                for c in range(3):
                    tap = [part[(a * 9 + b * 3 + c) * 16 : (a * 9 + b * 3 + c + 1) * 16] for a in range(3)]
                    row_taps[b].append((tap[0] + tap[1], tap[2]))
            taps.append(row_taps)

    def finish(sums):
        def shifted(value, c):
            if c == 0:
                return jnp.where(col == 0, value, pltpu.roll(value, 1, 1))
            if c == 2:
                return jnp.where(col == cols - 1, value, pltpu.roll(value, lanes - 1, 1))
            return value

        early = sum(shifted(sums[c][0], c) for c in range(3))
        late = sum(shifted(sums[c][1], c) for c in range(3))
        return late + jnp.where(in_first, early, pltpu.roll(early, cols, 1))

    def add(*parts):
        return [tuple(sum(p[c][k] for p in parts) for k in range(2)) for c in range(3)]

    def where(flag, one, other):
        return [
            tuple(jnp.where(flag, one[c][k], 0.0 if other is None else other[c][k]) for k in range(2))
            for c in range(3)
        ]

    out = []
    for row in range(rows):
        parts = [taps[row + b - 1][b] for b in range(3) if 0 <= row + b - 1 < rows]
        if row == 0:
            parts.append(where(is_first, taps[0][0], None))
        if row == rows - 1:
            parts.append(where(is_last, taps[rows - 1][2], None))
        out.append(finish(add(*parts)) + bias)
    if tiles == 2:
        return out, (finish(where(is_first, taps[rows - 1][0], taps[0][2])),), is_first
    return out, (finish(taps[rows - 1][0]), finish(taps[0][2])), is_first


def conv_pair_kernel(features_ref, weight_ref, bias_ref, send_ref, keep_ref, *scratch):
    out, (owed,), is_first = conv_rows(features_ref, weight_ref, bias_ref, *scratch, 2)
    rows = len(out)
    for row in range(rows):
        send_ref[row] = out[row].astype(BF16)
    edge = jnp.where(is_first, out[rows - 1], out[0])
    keep_ref[0] = edge
    keep_ref[1] = owed
    send_ref[rows] = (edge - edge.astype(BF16).astype(F32)).astype(BF16)
    high = owed.astype(BF16)
    send_ref[rows + 1] = high
    send_ref[rows + 2] = (owed - high.astype(F32)).astype(BF16)


def selection(lanes, cols):
    shape = (2 * lanes, 2 * lanes)
    src = lax.broadcasted_iota(jnp.int32, shape, 0)
    dst = lax.broadcasted_iota(jnp.int32, shape, 1)
    half = cols // 2
    x = dst // lanes
    f = dst % lanes // cols
    i = dst % cols // half
    j = dst % half
    want = i * lanes + f * cols + 2 * j + x
    return jnp.where(src == want, 1.0, 0.0).astype(BF16)


def to_tokens(latent_rows, cols):
    blocks = [
        jnp.concatenate([latent_rows[y], latent_rows[2 + y]], axis=1) for y in range(2)
    ]
    return jnp.concatenate(blocks, axis=0)


def finish_pair_kernel(send_ref, recv_ref, keep_ref, tokens_ref, *, cols):
    is_first = lax.axis_index("tile") == 0
    slots, zc, lanes = send_ref.shape
    rows = slots - 3
    mine = [send_ref[row].astype(F32) for row in range(rows)]
    theirs = [recv_ref[row].astype(F32) for row in range(rows)]
    my_edge = keep_ref[0] + (recv_ref[rows + 1].astype(F32) + recv_ref[rows + 2].astype(F32))
    their_edge = jnp.where(is_first, theirs[0], theirs[rows - 1]) + recv_ref[rows].astype(F32) + keep_ref[1]
    mine[0] = jnp.where(is_first, mine[0], my_edge)
    mine[rows - 1] = jnp.where(is_first, my_edge, mine[rows - 1])
    theirs[0] = jnp.where(is_first, their_edge, theirs[0])
    theirs[rows - 1] = jnp.where(is_first, theirs[rows - 1], their_edge)
    low = [jnp.where(is_first, a, b) for a, b in zip(mine, theirs)]
    high = [jnp.where(is_first, b, a) for a, b in zip(mine, theirs)]
    stacked = jnp.concatenate([to_tokens(low, cols), to_tokens(high, cols)], axis=0).astype(BF16)
    picked = jnp.dot(stacked, selection(lanes, cols), preferred_element_type=F32).astype(BF16)
    for t in range(2):
        for y in range(2):
            for x in range(2):
                tokens_ref[t, (2 * y + x) * zc : (2 * y + x + 1) * zc] = picked[
                    (2 * t + y) * zc : (2 * t + y + 1) * zc, x * lanes : (x + 1) * lanes
                ]


def conv_any_kernel(features_ref, weight_ref, bias_ref, part_ref, owed_ref, *scratch, tiles):
    out, owed, _ = conv_rows(features_ref, weight_ref, bias_ref, *scratch, tiles)
    for row, value in enumerate(out):
        part_ref[row] = value
    owed_ref[0] = owed[0]
    owed_ref[1] = owed[1]


def finish_any_kernel(part_ref, from_low_ref, from_high_ref, tokens_ref, *, cols):
    rows, zc, lanes = part_ref.shape
    latent = [part_ref[row] for row in range(rows)]
    latent[0] = latent[0] + from_low_ref[...]
    latent[rows - 1] = latent[rows - 1] + from_high_ref[...]
    stacked = to_tokens(latent, cols).astype(BF16)
    picked = jnp.dot(stacked, selection(lanes, cols), preferred_element_type=F32).astype(BF16)
    for y in range(2):
        for x in range(2):
            tokens_ref[(2 * y + x) * zc : (2 * y + x + 1) * zc] = picked[
                y * zc : (y + 1) * zc, x * lanes : (x + 1) * lanes
            ]


def prepare_kernel(bucket_ref, frames_ref, embed_ref, qgain_ref, kgain_ref, slot_ref, key_t_ref, qscale_ref, kscale_ref):
    seq = lax.axis_index("seq")
    me = lax.axis_index("group")
    src = [jnp.int32(0)] * CAP
    count = jnp.int32(0)
    for g in range(bucket_ref.shape[1]):
        hit = bucket_ref[seq, g] == me
        for slot in range(CAP):
            src[slot] = jnp.where(hit & (count == slot), g, src[slot])
        count = count + jnp.where(hit, 1, 0)
    for slot in range(CAP):
        slot_ref[0, slot] = src[slot]
        slot_ref[1, slot] = jnp.where(count > slot, frames_ref[seq, src[slot]], 0)
    key_t_ref[...] = jnp.transpose(embed_ref[:, D : 2 * D].astype(F32)).astype(BF16)
    qscale_ref[...] = qgain_ref[...] * math.log2(math.e)
    kscale_ref[...] = jnp.broadcast_to(column(kgain_ref[...]) * math.sqrt(HEAD), kscale_ref.shape)


def attend_kernel(slot_ref, *refs, sources, cols):
    token_refs = refs[:sources]
    embed_ref, key_t_ref, qscale_ref, kscale_ref, out_ref = refs[sources : 5 + sources]
    nat_scr, tr_scr, k_scr, q_scr, v_scr, p_scr, r_scr, out_scr, sem = refs[5 + sources :]
    me = lax.axis_index("group")
    tile = lax.axis_index("tile")
    tiles, _, lanes = token_refs[0].shape[-3:]
    frame_lane = lax.broadcasted_iota(jnp.int32, (1, lanes), 1) // cols
    frame_row = lax.broadcasted_iota(jnp.int32, (lanes, 1), 0) // cols
    counted, row_keep = {}, {}

    def load(slot):
        source = slot_ref[0, slot]
        total = slot_ref[1, slot]
        if sources == 1:
            raw = token_refs[0][source].astype(F32)
        else:
            raw = token_refs[0][...].astype(F32)
            for k in range(1, sources):
                raw = jnp.where((source ^ me) == k, token_refs[k][...].astype(F32), raw)
        valid = jnp.where(frame_lane < total, 1.0, 0.0)
        counted[slot] = jnp.where(frame_lane < jnp.maximum(total, 1), 1.0, 0.0)
        row_keep[slot] = jnp.where(frame_row < total, 1.0, 0.0)
        tokens_t = jnp.concatenate([raw[t] * valid for t in range(tiles)], axis=1)
        tr_scr[slot] = tokens_t.astype(BF16)
        nat_scr[slot] = jnp.transpose(tokens_t).astype(BF16)

    pairs = HEADS // 2

    def project_k(step, half):
        slot, pair = divmod(step, pairs)
        start = (2 * pair + half) * HEAD
        k = jnp.dot(key_t_ref[start : start + HEAD, :], tr_scr[slot], preferred_element_type=F32)
        k = k * lax.rsqrt(jnp.sum(k * k, axis=0, keepdims=True) + HEAD * EPS) * kscale_ref[...]
        k_scr[step % 2, half] = k.astype(BF16)

    def project_q(step):
        slot, pair = divmod(step, pairs)
        span = slice(pair * 2 * HEAD, (pair + 1) * 2 * HEAD)
        mine = nat_scr[slot, pl.ds(pl.multiple_of(tile * lanes, lanes), lanes), :]
        queries = jnp.dot(mine, embed_ref[:, span], preferred_element_type=F32)
        for half in range(2):
            q = queries[:, half * HEAD : (half + 1) * HEAD]
            q = q * lax.rsqrt(jnp.sum(q * q, axis=1, keepdims=True) + HEAD * EPS) * qscale_ref[...]
            q_scr[step % 2, half] = q.astype(BF16)

    def project_v(step):
        slot, pair = divmod(step, pairs)
        start = 2 * D + pair * 2 * HEAD
        v_scr[step % 3] = jnp.dot(
            nat_scr[slot], embed_ref[:, start : start + 2 * HEAD], preferred_element_type=F32
        ).astype(BF16)

    def score(step, half):
        slot = step // pairs
        scores = jnp.dot(q_scr[step % 2, half], k_scr[step % 2, half], preferred_element_type=F32)
        weights = jnp.exp2(scores)
        p_scr[step % 2, half] = weights.astype(BF16)
        folded = weights[:, :lanes]
        for t in range(1, tiles):
            folded = folded + weights[:, t * lanes : (t + 1) * lanes]
        totals = jnp.sum(folded * counted[slot], axis=1, keepdims=True)
        r_scr[step % 2, half] = jnp.broadcast_to(row_keep[slot] / totals, (lanes, HEAD))

    def mix(step, half):
        slot, pair = divmod(step, pairs)
        start = (2 * pair + half) * HEAD
        mixed = jnp.dot(
            p_scr[step % 2, half], v_scr[step % 3, :, half * HEAD : (half + 1) * HEAD], preferred_element_type=F32
        )
        out_scr[slot, :, start : start + HEAD] = (mixed * r_scr[step % 2, half]).astype(BF16)
        if half == 1:
            part = (slot, slice(None), pl.ds(pair * 2 * HEAD, 2 * HEAD))
            copies.append(pltpu.make_async_copy(out_scr.at[part], out_ref.at[part], sem.at[step]))
            copies[-1].start()

    copies = []

    def run(slots):
        steps = slots * pairs
        load(0)
        for slot in range(slots, CAP):
            out_scr[slot] = jnp.zeros(out_scr.shape[1:], BF16)
            copies.append(pltpu.make_async_copy(out_scr.at[slot], out_ref.at[slot], sem.at[slot * pairs]))
            copies[-1].start()
        for step in range(steps + 2):
            here, last, before = step < steps, 1 <= step <= steps, step >= 2
            if here:
                project_q(step)
                project_k(step, 0)
                project_k(step, 1)
                project_v(step)
            if last:
                score(step - 1, 0)
                score(step - 1, 1)
            if before:
                mix(step - 2, 0)
                mix(step - 2, 1)
            if step < steps and step % pairs == 2 and slots > step // pairs + 1:
                load(step // pairs + 1)
        for copy in copies:
            copy.wait()
        copies.clear()

    double = slot_ref[1, CAP - 1] > 0

    @pl.when(double)
    def _():
        run(CAP)

    @pl.when(jnp.logical_not(double))
    def _():
        run(1)


def clip_tokens(features, weight_t, bias_row):
    _, _, frames, rows, cols, channels = features.shape
    zc = bias_row.shape[1]
    lanes = frames * cols
    tiles = lax.axis_size("tile")
    scratch = [
        pltpu.VMEM((rows, frames, cols, channels), BF16),
        pltpu.VMEM(weight_t.shape, BF16),
        pltpu.VMEM(bias_row.shape, F32),
        pltpu.SemaphoreType.DMA((rows,)),
        pltpu.SemaphoreType.DMA,
        pltpu.SemaphoreType.DMA,
    ]
    if tiles == 2:
        send, keep = pl.pallas_call(
            conv_pair_kernel,
            out_shape=(pltpu.VMEM((rows + 3, zc, lanes), BF16), pltpu.VMEM((2, zc, lanes), F32)),
            in_specs=[HBM, HBM, HBM],
            out_specs=(VMEM, VMEM),
            scratch_shapes=scratch,
            name="conv",
        )(features, weight_t, bias_row)
        recv = lax.ppermute(send, "tile", [(0, 1), (1, 0)])
        return pl.pallas_call(
            functools.partial(finish_pair_kernel, cols=cols),
            out_shape=pltpu.VMEM((2, 4 * zc, lanes), BF16),
            in_specs=[VMEM, VMEM, VMEM],
            out_specs=VMEM,
            name="finish",
        )(*in_vmem(send, recv, keep))
    part, owed = pl.pallas_call(
        functools.partial(conv_any_kernel, tiles=tiles),
        out_shape=(pltpu.VMEM((rows, zc, lanes), F32), pltpu.VMEM((2, zc, lanes), F32)),
        in_specs=[HBM, HBM, HBM],
        out_specs=(VMEM, VMEM),
        scratch_shapes=scratch,
        name="conv",
    )(features, weight_t, bias_row)
    up = [(i, i + 1) for i in range(tiles - 1)]
    from_low = lax.ppermute(owed[0], "tile", up)
    from_high = lax.ppermute(owed[1], "tile", [(b, a) for a, b in up])
    tokens = pl.pallas_call(
        functools.partial(finish_any_kernel, cols=cols),
        out_shape=pltpu.VMEM((4 * zc, lanes), BF16),
        in_specs=[VMEM, VMEM, VMEM],
        out_specs=VMEM,
        name="finish",
    )(*in_vmem(part, from_low, from_high))
    return lax.all_gather(tokens, "tile", axis=0)


def shards(features, conv_weight, conv_bias, embed_qkv, query_gain, key_gain, bucket, frames):
    _, _, frame_count, rows, cols, channels = features.shape
    zc = conv_weight.shape[-1]
    lanes = frame_count * cols
    tiles = lax.axis_size("tile")
    groups = lax.axis_size("group")
    weight_t = jnp.transpose(conv_weight, (0, 1, 2, 4, 3)).reshape(-1, channels)
    tokens = clip_tokens(features, weight_t, conv_bias.reshape(1, -1))
    (embed,) = in_vmem(embed_qkv)
    slots, key_t, query_scale, key_scale = pl.pallas_call(
        prepare_kernel,
        out_shape=(
            pltpu.SMEM((2, CAP), jnp.int32),
            pltpu.VMEM((D, 4 * zc), BF16),
            pltpu.VMEM((1, HEAD), F32),
            pltpu.VMEM((HEAD, tiles * lanes), F32),
        ),
        in_specs=[SMEM, SMEM, VMEM, VMEM, VMEM],
        out_specs=(SMEM, VMEM, VMEM, VMEM),
        name="prepare",
    )(bucket, frames, embed, query_gain.reshape(1, -1), key_gain.reshape(1, -1))
    if groups in (2, 4):
        sources = [tokens] + [
            lax.ppermute(tokens, "group", [(i, i ^ k) for i in range(groups)]) for k in range(1, groups)
        ]
    else:
        sources = [lax.all_gather(tokens, "group", axis=0)]
    clip = tiles * lanes
    out = pl.pallas_call(
        functools.partial(attend_kernel, sources=len(sources), cols=cols),
        out_shape=jax.ShapeDtypeStruct((CAP, lanes, D), BF16),
        in_specs=[SMEM] + [VMEM] * (len(sources) + 4),
        out_specs=HBM,
        scratch_shapes=[
            pltpu.VMEM((CAP, clip, 4 * zc), BF16),
            pltpu.VMEM((CAP, 4 * zc, clip), BF16),
            pltpu.VMEM((2, 2, HEAD, clip), BF16),
            pltpu.VMEM((2, 2, lanes, HEAD), BF16),
            pltpu.VMEM((3, clip, 2 * HEAD), BF16),
            pltpu.VMEM((2, 2, lanes, clip), BF16),
            pltpu.VMEM((2, 2, lanes, HEAD), F32),
            pltpu.VMEM((CAP, lanes, D), BF16),
            pltpu.SemaphoreType.DMA((CAP * HEADS // 2,)),
        ],
        name="attend",
    )(pltpu.with_memory_space_constraint(slots, pltpu.SMEM), *in_vmem(*sources, embed, key_t, query_scale, key_scale))
    return out[None, None]


def solution(mesh):
    in_specs = (P("seq", "group", None, "tile", None, None), P(), P(), P(), P(), P(), P(), P())
    out_specs = P("seq", "group", None, "tile", None)
    return jax.shard_map(shards, mesh=mesh, in_specs=in_specs, out_specs=out_specs, check_vma=False)
```
